16 devices in a mesh: f: 2 (over z), h: 8 (over y, x, core).
Axes of the slice: x: 2, y: 2, z: 2, core: 2. Of those that a mesh axis runs over, the one named last changes fastest.
Arguments:
- x: bfloat16 [4096, 3072], P(None, 'h')
- g1: float32 [3072], P('h')
- g2: float32 [3072], P('h')
- w_gate: bfloat16 [3072, 8192], P('h', 'f')
- w_up: bfloat16 [3072, 8192], P('h', 'f')
- w_down: bfloat16 [8192, 3072], P('f', 'h')
- o: bfloat16 [4096, 3072], P(None, 'f')
- w_o: bfloat16 [3072, 3072], P('f', 'h')
- w_qkv: bfloat16 [3072, 5120], P('h', 'f')
Outputs:
- output 1: bfloat16 [4096, 3072], P(None, 'h')
- output 2: bfloat16 [4096, 5120], P(None, 'f')
All inputs are finite; a program needn't handle non-finite values.
Results may differ from the reference program's by a relative error of at most 0.0039825.
Values are sent between devices in bfloat16 or wider.
A program may use at most 1 GiB of HBM per device.

```python
import jax
import jax.numpy as jnp
from jax import lax

T = 4096
D = 3072
FF = 8192
HEADS = 24
KV_HEADS = 8
HEAD = 128
HD = HEADS * HEAD
Q = (HEADS + 2 * KV_HEADS) * HEAD
EPS = 1e-6


def _w(key, shape):
    return (jax.random.normal(key, shape, jnp.float32) * shape[0] ** -0.5).astype(jnp.bfloat16)


def setup_inputs(seed: int = 0) -> dict:
    ks = jax.random.split(jax.random.PRNGKey(seed), 11)
    z = jax.random.normal(ks[0], (T, D), jnp.float32)
    row = jnp.exp(jax.random.uniform(ks[1], (T, 1), jnp.float32, -1.0, 1.0))
    tilt = jax.random.uniform(ks[2], (T, 1), jnp.float32, -1.0, 1.0)
    pos = jnp.arange(D, dtype=jnp.float32)[None, :] * (2.0 / D) - 1.0
    x = (z * row * jnp.exp(tilt * pos)).astype(jnp.bfloat16)
    o = (0.7 * jax.random.normal(ks[8], (T, HD), jnp.float32)).astype(jnp.bfloat16)
    return {
        'x': x,
        'g1': jax.random.uniform(ks[3], (D,), jnp.float32, 0.5, 1.5),
        'g2': jax.random.uniform(ks[4], (D,), jnp.float32, 0.5, 1.5),
        'w_gate': _w(ks[5], (D, FF)),
        'w_up': _w(ks[6], (D, FF)),
        'w_down': _w(ks[7], (FF, D)),
        'o': o,
        'w_o': _w(ks[9], (HD, D)),
        'w_qkv': _w(ks[10], (D, Q)),
    }


def _norm(x, g):
    xf = x.astype(jnp.float32)
    r = lax.rsqrt(jnp.mean(xf * xf, axis=-1, keepdims=True) + EPS)
    return (xf * r * g).astype(jnp.bfloat16)


def reference(x, g1, g2, w_gate, w_up, w_down, o, w_o, w_qkv):
    n = _norm(x, g1)
    gt = jnp.dot(n, w_gate, preferred_element_type=jnp.float32)
    up = jnp.dot(n, w_up, preferred_element_type=jnp.float32)
    a = (jax.nn.silu(gt) * up).astype(jnp.bfloat16)
    y = jnp.dot(a, w_down, preferred_element_type=jnp.float32) + jnp.dot(o, w_o, preferred_element_type=jnp.float32)
    x_next = (x.astype(jnp.float32) + y).astype(jnp.bfloat16)
    n1 = _norm(x_next, g2)
    qkv = jnp.dot(n1, w_qkv, preferred_element_type=jnp.float32).astype(jnp.bfloat16)
    return (x_next, qkv)
```

```python
import jax
import jax.numpy as jnp
from jax import lax
from jax.sharding import PartitionSpec as P

EPS = 1e-6
PIECES = 4
CHUNKS = 4


def _dot(a, b):
    return jnp.dot(a, b, preferred_element_type=jnp.float32)


def _rms(x, g):
    xf = x.astype(jnp.float32)
    ss = jnp.sum(xf * xf, axis=-1, keepdims=True)
    return (xf * lax.rsqrt(ss / x.shape[1] + EPS) * g).astype(jnp.bfloat16)


def _swap(v, bit):
    return lax.ppermute(v, 'h', [(i, i ^ bit) for i in range(8)])


def _zswap(v):
    return lax.ppermute(v, 'f', [(0, 1), (1, 0)])


def _rows(v, start, size):
    return lax.dynamic_slice_in_dim(v, start, size, 0)


def _cols(v, start, size):
    return lax.dynamic_slice_in_dim(v, start, size, 1)


def _pair(first, own, other, axis):
    lo = jnp.where(first, own, other)
    hi = jnp.where(first, other, own)
    return jnp.concatenate([lo, hi], axis)


C, X, Y = 1, 2, 4


def solution(mesh):
    def body(x, g1, g2, w_gate, w_up, w_down, o, w_o, w_qkv):
        h = lax.axis_index('h')
        z = lax.axis_index('f')
        iy, ix, ic = h // 4, (h // 2) % 2, h % 2
        t, d = x.shape
        q = t // 4

        g = jnp.stack([g1, g2])
        for bit in (X, Y, C):
            g = jnp.concatenate([g, _swap(g, bit)], 1)

        xc = jnp.concatenate([_rows(x, ic * 2 * q, 2 * q), _swap(_rows(x, (1 - ic) * 2 * q, 2 * q), C)], 1)
        xy = _rows(xc, iy * q, q)
        yy = _swap(_rows(xc, (1 - iy) * q, q), Y)
        m = jnp.concatenate([xy, yy], 1)
        mx = _swap(m, X)
        parts = []
        for kc in range(2):
            for ky in range(2):
                b = (2 * ky + kc) * d
                parts += [m[:, b:b + d], mx[:, b:b + d]]
        full = jnp.concatenate(parts, 1)
        n = _rms(full, g[0])

        def gather_w(w):
            half = w.shape[1] // 2
            s = jnp.concatenate([_cols(w, ix * half, half), _swap(_cols(w, (1 - ix) * half, half), X)], 0)
            s = jnp.concatenate([s, _swap(s, Y)], 0)
            return jnp.concatenate([s, _swap(s, C)], 0)

        ff = w_gate.shape[1]
        p = ff // 2 // PIECES
        acts, acts_x = [], []
        for j in range(PIECES):
            cols = lambda w: jnp.concatenate([w[:, j * p:(j + 1) * p], w[:, ff // 2 + j * p:ff // 2 + (j + 1) * p]], 1)
            wg, wu = gather_w(cols(w_gate)), gather_w(cols(w_up))
            a = (jax.nn.silu(_dot(n, wg)) * _dot(n, wu)).astype(jnp.bfloat16)
            acts.append(a)
            acts_x.append(_swap(a, X))
        act = jnp.concatenate(acts + acts_x, 1)

        def cols_group(w):
            s = jnp.concatenate([w, _swap(w, Y)], 1)
            return jnp.concatenate([s, _swap(s, C)], 1)

        wd_rel = jnp.concatenate([_rows(w_down, ix * (ff // 2), ff // 2), _rows(w_down, (1 - ix) * (ff // 2), ff // 2)], 0)
        wd, wo = cols_group(wd_rel), cols_group(w_o)
        o_my = _rows(o, (ic * 2 + iy) * q, q)
        wq = gather_w(w_qkv)

        res = jnp.concatenate([full[:, (2 * k) * d:(2 * k + 1) * d] for k in range(4)], 1)
        r = q // CHUNKS
        xs, qs = [], []
        hr = r // 2
        for i in range(CHUNKS):
            sl = slice(i * r, (i + 1) * r)
            y = _dot(act[sl], wd) + _dot(o_my[sl], wo)
            mine = _rows(y, z * hr, hr) + _zswap(_rows(y, (1 - z) * hr, hr))
            xz = (_rows(res[sl], z * hr, hr).astype(jnp.float32) + mine).astype(jnp.bfloat16)
            xo = _zswap(xz)
            xg = _pair(z == 0, xz, xo, 0)
            xs.append(xg)
            xx = _swap(xg, X)
            nf = jnp.concatenate([v[:, k * d:(k + 1) * d] for k in range(4) for v in (xg, xx)], 1)
            qs.append(_dot(_rms(nf, g[1]), wq).astype(jnp.bfloat16))
        xn = jnp.concatenate(xs, 0)
        own_y = jnp.concatenate([xn[:, :d], xn[:, 2 * d:3 * d]], 1)
        oth_y = jnp.concatenate([xn[:, d:2 * d], xn[:, 3 * d:]], 1)
        xh = _pair(iy == 0, own_y, _swap(oth_y, Y), 0)
        x_out = _pair(ic == 0, xh[:, :d], _swap(xh[:, d:], C), 0)

        outs = []
        for v in qs:
            v = _pair(ix == 0, v, _swap(v, X), 1)
            outs.append((v, _swap(v, Y)))
        mine = jnp.concatenate([v for v, _ in outs], 0)
        other = jnp.concatenate([v for _, v in outs], 0)
        half = _pair(iy == 0, mine, other, 0)
        qkv = _pair(ic == 0, half, _swap(half, C), 0)
        return x_out, qkv

    in_specs = (P(None, 'h'), P('h'), P('h'), P('h', 'f'), P('h', 'f'), P('f', 'h'),
                P(None, 'f'), P('f', 'h'), P('h', 'f'))
    return jax.shard_map(body, mesh=mesh, in_specs=in_specs,
                         out_specs=(P(None, 'h'), P(None, 'f')), check_vma=False)
```

```python
import jax
import jax.numpy as jnp
from jax import lax
from jax.experimental import pallas as pl
from jax.experimental.pallas import tpu as pltpu
from jax.sharding import PartitionSpec as P

EPS = 1e-6
BF, F32 = jnp.bfloat16, jnp.float32
MESH = pl.DeviceIdType.MESH
NREMOTE, NLOCAL = 176, 96

T, D, FF, HD, Q = 4096, 3072, 8192, 3072, 5120
B = D // 8
R = T // 4
Z = R // 2
FP = FF // 2
PIECES = 4
PC = FP // 2 // PIECES
K2 = FP + HD // 2
S = 128
QC = Q // 4
CH = 256


def _dot(a, b):
    return jnp.dot(a, b, preferred_element_type=F32)


def _kernel(x, g, wg, wu, wd, o, wo, wq, xo, qo, dl, ql,
            A, N, W, act, ys, yr, yo, gv, send, recv, loc):
    h = lax.axis_index('h')
    z = lax.axis_index('f')
    iy, ix, ic = lax.div(h, 4), lax.rem(lax.div(h, 2), 2), lax.rem(h, 2)

    def dev(kx, ky, kc):
        py = 1 - iy if ky else iy
        px = 1 - ix if kx else ix
        pc = 1 - ic if kc else ic
        return {'h': py * 4 + px * 2 + pc}

    XN, YN, CN, YCN, ZN = dev(1, 0, 0), dev(0, 1, 0), dev(0, 0, 1), dev(0, 1, 1), {'f': 1 - z}
    count = [0, 0]
    sends = []

    def put(src, dst, to):
        i = count[0]
        count[0] += 1
        c = pltpu.make_async_remote_copy(src, dst, send.at[i], recv.at[i], device_id=to, device_id_type=MESH)
        c.start()
        sends.append(c)
        return c

    def load(src, dst):
        i = count[1]
        count[1] += 1
        c = pltpu.make_async_copy(src, dst, loc.at[i])
        c.start()
        return c

    def settle(cs):
        for c in cs:
            c.wait_send()
            sends[:] = [d for d in sends if d is not c]

    def al(v, m):
        return pl.multiple_of(v, m)

    def ds(start, size, m):
        return pl.ds(al(start, m), size)

    def quarter(py, pc):
        return pc * (2 * R) + py * R

    mine = quarter(iy, ic)
    zr = ds(z * Z, Z, Z)
    zo = ds((1 - z) * Z, Z, Z)

    bar = pltpu.get_barrier_semaphore()
    for k in range(1, 8):
        pl.semaphore_signal(bar, inc=1, device_id=dev(k & 1, (k >> 1) & 1, k >> 2), device_id_type=MESH)
    pl.semaphore_signal(bar, inc=1, device_id=ZN, device_id_type=MESH)
    pl.semaphore_wait(bar, 8)

    def col(p):
        return pl.ds(p * B, B)

    x4 = put(x.at[ds(quarter(iy, 1 - ic), R, R), :], A.at[:, col(4)], CN)
    x2 = put(x.at[ds(quarter(1 - iy, ic) + z * Z, Z, Z), :], A.at[zr, col(2)], YN)
    x6 = put(x.at[ds(quarter(1 - iy, 1 - ic) + z * Z, Z, Z), :], A.at[zr, col(6)], YCN)
    x1 = put(x.at[ds(mine + z * Z, Z, Z), :], A.at[zr, col(1)], XN)
    x0 = load(x.at[ds(mine, R, R), :], A.at[:, col(0)])

    def wrow(j, a, n):
        return pl.ds(j * D + a, n)

    wl, wx, wyo, wyf, wc = {}, {}, {}, {}, {}

    def w_load(j):
        c0 = ds(ix * (FP // 2) + j * PC, PC, PC)
        wl[j] = [load(wg.at[:, c0], W.at[wrow(j, 0, B), pl.ds(0, PC)]),
                 load(wu.at[:, c0], W.at[wrow(j, 0, B), pl.ds(PC, PC)])]

    def w_x(j):
        c1 = ds((1 - ix) * (FP // 2) + j * PC, PC, PC)
        wx[j] = [put(wg.at[:, c1], W.at[wrow(j, B, B), pl.ds(0, PC)], XN),
                 put(wu.at[:, c1], W.at[wrow(j, B, B), pl.ds(PC, PC)], XN)]

    def w_yown(j):
        for c in wl[j]:
            c.wait()
        wyo[j] = put(W.at[wrow(j, 0, B), :], W.at[wrow(j, 2 * B, B), :], YN)

    def w_xgot(j):
        for c in wx[j]:
            c.wait_recv()
        wyf[j] = put(W.at[wrow(j, B, B), :], W.at[wrow(j, 3 * B, B), :], YN)
        wc[j] = [put(W.at[wrow(j, 0, 2 * B), :], W.at[wrow(j, 4 * B, 2 * B), :], CN)]

    def w_ygot(j):
        wyo[j].wait_recv()
        wc[j].append(put(W.at[wrow(j, 2 * B, B), :], W.at[wrow(j, 6 * B, B), :], CN))
        wyf[j].wait_recv()
        wc[j].append(put(W.at[wrow(j, 3 * B, B), :], W.at[wrow(j, 7 * B, B), :], CN))

    for j in range(PIECES):
        w_load(j)
    w_x(0)
    gs = [put(g, gv.at[:, col(k)], dev(k & 1, (k >> 1) & 1, k >> 2)) for k in range(1, 8)]
    g0 = load(g, gv.at[:, col(0)])
    w_yown(0)
    w_yown(1)
    ol = load(o.at[ds(mine, R, R), :], act.at[:, pl.ds(FP, HD // 2)])

    dc = [put(wd, dl.at[1, pl.ds(0, FP), :], CN), put(wo, dl.at[1, pl.ds(FP, HD // 2), :], CN)]
    qc0 = put(wq.at[:, ds(ix * QC, QC, QC)], ql.at[4], CN)

    x4.wait_recv()
    x5 = put(A.at[zr, col(4)], A.at[zr, col(5)], XN)
    zs = []

    def zput(p):
        zs.append(put(A.at[zr, col(p)], A.at[zr, col(p)], ZN))

    x1.wait_recv()
    zput(1)
    x2.wait_recv()
    x3 = put(A.at[zr, col(2)], A.at[zr, col(3)], XN)
    zput(2)
    x6.wait_recv()
    x7 = put(A.at[zr, col(6)], A.at[zr, col(7)], XN)
    zput(6)
    for j in range(1, PIECES):
        w_x(j)
    w_xgot(0)
    w_yown(2)
    x5.wait_recv()
    zput(5)
    x3.wait_recv()
    zput(3)
    x7.wait_recv()
    zput(7)
    for c in gs:
        c.wait_recv()
    g0.wait()
    x0.wait()
    for c in zs:
        c.wait_recv()

    def norm(row, n, gi):
        gain = gv[gi:gi + 1, :]

        def body(i, _):
            rows = ds(row + i * 32, 32, 32)
            v = A[rows, :].astype(F32)
            ss = jnp.sum(v * v, axis=-1, keepdims=True)
            N[rows, :] = (v * lax.rsqrt(ss / D + EPS) * gain).astype(BF)
            return 0

        lax.fori_loop(0, n // 32, body, 0)

    norm(0, R, 0)

    def gate_up(j):
        def body(t, _):
            rows = ds(lax.div(t, 2) * 256, 256, 256)
            c = lax.rem(t, 2) * 256
            n = N[rows, :]
            gt = _dot(n, W[wrow(j, 0, D), ds(c, 256, 256)])
            up = _dot(n, W[wrow(j, 0, D), ds(PC + c, 256, 256)])
            act[rows, ds(j * PC + c, 256, 256)] = (jax.nn.silu(gt) * up).astype(BF)
            return 0

        lax.fori_loop(0, (R // 256) * (PC // 256), body, 0)

    dy = {}

    def down_y(p):
        c = pl.ds(p * S, S)
        dy[p] = [put(wd.at[:, c], dl.at[0, pl.ds(0, FP), c], YN),
                 put(wo.at[:, c], dl.at[0, pl.ds(FP, HD // 2), c], YN)]

    acts = []
    for j in range(PIECES):
        if j + 1 < PIECES:
            w_xgot(j + 1)
        if j == 0:
            w_yown(3)
        if j == 2:
            for p in range(3):
                down_y(p)
        w_ygot(j)
        for c in wc[j]:
            c.wait_recv()
        gate_up(j)
        if j == 0:
            settle(zs + [x1, x2, x3, x4, x5, x6, x7] + gs)
        acts.append(put(act.at[:, pl.ds(j * PC, PC)], act.at[:, pl.ds(FP // 2 + j * PC, PC)], XN))

    qx = put(wq.at[:, ds((1 - ix) * QC, QC, QC)], ql.at[1], XN)
    qy = put(wq.at[:, ds(ix * QC, QC, QC)], ql.at[2], YN)

    for j in range(PIECES):
        settle(wx[j] + [wyo[j], wyf[j]] + wc[j])

    def down_load(ky, p):
        out = []
        for kc in range(2):
            c = pl.ds(p * S, S)
            if ky == 0 and kc == 0:
                top, bot = wd, wo.at[:, c]
            else:
                k = {(1, 0): 0, (0, 1): 1, (1, 1): 2}[ky, kc]
                top, bot = dl.at[k], dl.at[k, pl.ds(FP, HD // 2), c]
            to = pl.ds(p * 2 * S + kc * S, S)
            r0 = ky * K2
            out.append(load(top.at[ds(ix * (FP // 2), FP // 2, FP // 2), c], W.at[pl.ds(r0, FP // 2), to]))
            out.append(load(top.at[ds((1 - ix) * (FP // 2), FP // 2, FP // 2), c], W.at[pl.ds(r0 + FP // 2, FP // 2), to]))
            out.append(load(bot, W.at[pl.ds(r0 + FP, HD // 2), to]))
        return out

    for c in dc:
        c.wait_recv()
    dloads = {p: down_load(0, p) for p in range(3)}
    ol.wait()
    for c in acts:
        c.wait_recv()

    rs = {}

    def down(ky, p):
        s = (ky * 3 + p) * 2 * S
        w = lambda: W[pl.ds(ky * K2, K2), pl.ds(p * 2 * S, 2 * S)]

        def body(base, dst):
            def f(i, _):
                dst[ds(i * 256, 256, 256), pl.ds(s, 2 * S)] = _dot(act[ds(base + i * 256, 256, 256), :], w())
                return 0
            lax.fori_loop(0, Z // 256, f, 0)

        body((1 - z) * Z, ys)
        rs[ky, p] = put(ys.at[:, pl.ds(s, 2 * S)], yr.at[:, pl.ds(s, 2 * S)], ZN)
        body(z * Z, yo)

    def acol(ky, p, kc, kx=0):
        return pl.ds((2 * ky + 4 * kc + kx) * B + p * S, S)

    def finish(ky, p):
        rs[ky, p].wait_recv()

        def f(i, _):
            r = ds(i * 64, 64, 64)
            ra = ds(z * Z + i * 64, 64, 64)
            for kc in range(2):
                s = pl.ds((ky * 3 + p) * 2 * S + kc * S, S)
                c = acol(ky, p, kc)
                A[ra, c] = (A[ra, c].astype(F32) + (yo[r, s] + yr[r, s])).astype(BF)
            return 0

        lax.fori_loop(0, Z // 64, f, 0)

    xx, xz, xf = {}, {}, {}

    def share(ky, p):
        for kc in range(2):
            own, far = acol(ky, p, kc), acol(ky, p, kc, 1)
            xx[ky, p, kc] = put(A.at[zr, own], A.at[zr, far], XN)
            xz[ky, p, kc] = put(A.at[zr, own], A.at[zr, own], ZN)

    def forward(ky, p):
        for kc in range(2):
            own, far = acol(ky, p, kc), acol(ky, p, kc, 1)
            if ky == 0:
                xx[ky, p, kc].wait_recv()
                xf[ky, p, kc] = put(A.at[zr, far], A.at[zr, far], ZN)
            else:
                xz[ky, p, kc].wait_recv()
                xf[ky, p, kc] = put(A.at[zo, own], A.at[zo, far], XN)

    dyc = {}

    def down_ygot(p):
        for c in dy[p]:
            c.wait_recv()
        c = pl.ds(p * S, S)
        dyc[p] = put(dl.at[0, :, c], dl.at[2, :, c], CN)

    def down_ready(p):
        dyc[p].wait_recv()
        dloads[3 + p] = down_load(1, p)

    for p in range(3):
        for c in dloads[p]:
            c.wait()
        down(0, p)
    qx.wait_recv()
    qyf = put(ql.at[1], ql.at[3], YN)
    qc1 = put(ql.at[1], ql.at[5], CN)
    down_ygot(0)
    finish(0, 0)
    share(0, 0)
    down_ready(0)
    finish(0, 1)
    share(0, 1)
    forward(0, 0)
    for c in dloads[3]:
        c.wait()
    down(1, 0)
    finish(0, 2)
    share(0, 2)
    forward(0, 1)
    down_ygot(1)
    down_ready(1)
    finish(1, 0)
    share(1, 0)
    for c in dloads[4]:
        c.wait()
    down(1, 1)
    forward(0, 2)
    forward(1, 0)
    finish(1, 1)
    share(1, 1)
    down_ygot(2)
    down_ready(2)
    forward(1, 1)
    for c in dloads[5]:
        c.wait()
    down(1, 2)

    qy.wait_recv()
    qc2 = put(ql.at[2], ql.at[6], CN)
    finish(1, 2)
    share(1, 2)

    orow = ds(mine + z * Z, Z, Z)
    oy = put(A.at[zr, col(2)], xo.at[orow, :], YN)
    oyc = put(A.at[zr, col(6)], xo.at[orow, :], YCN)
    forward(1, 2)

    qyf.wait_recv()
    qc3 = put(ql.at[3], ql.at[7], CN)

    def qkv_load(k, src):
        return [load(src.at[:, pl.ds(0, 1024)], W.at[pl.ds(k * B, B), :]),
                load(src.at[:, pl.ds(1024, QC - 1024)], W.at[pl.ds(D + k * B, B), pl.ds(768, QC - 1024)])]

    qloads = []
    qloads += qkv_load(0, wq.at[:, ds(ix * QC, QC, QC)])
    for k in range(1, 4):
        qloads += qkv_load(k, ql.at[k])
    for k, c in zip(range(4, 8), (qc0, qc1, qc2, qc3)):
        c.wait_recv()
        qloads += qkv_load(k, ql.at[k])

    for p in range(3):
        for kc in range(2):
            xx[1, p, kc].wait_recv()
    for c in qloads:
        c.wait()
    settle(acts)

    xcol, ocol = ix * QC, (1 - ix) * QC
    qown, qxr, qyr, qdr, qcr = {}, {}, {}, {}, []

    def orows(py, pc, i):
        base = z * Z if i < 2 else (1 - z) * Z
        return ds(quarter(py, pc) + base + (i % 2) * CH, CH, CH)

    def at(rows, c):
        return qo.at[rows, ds(c, QC, QC)]

    def qkv_chunk(i):
        base = (z * Z if i < 2 else (1 - z) * Z) + (i % 2) * CH
        norm(base, CH, 1)
        rows = ds(base, CH, CH)

        def f(t, _):
            act[rows, ds(t * 256, 256, 256)] = _dot(N[rows, :], W[pl.ds(0, D), ds(t * 256, 256, 256)]).astype(BF)
            return 0

        lax.fori_loop(0, 4, f, 0)
        act[rows, pl.ds(1024, 256)] = _dot(N[rows, :], W[pl.ds(D, D), pl.ds(768, 256)]).astype(BF)
        src = act.at[rows, pl.ds(0, QC)]
        dst = at(orows(iy, ic, i), xcol)
        qxr[i] = put(src, dst, XN)
        qyr[i] = put(src, dst, YN)
        qcr.append(put(src, dst, CN))
        qown[i] = load(src, dst)

    qkv_chunk(0)
    qkv_chunk(1)
    for p in range(3):
        for kc in range(2):
            xz[0, p, kc].wait_recv()
            xf[0, p, kc].wait_recv()
            xf[1, p, kc].wait_recv()
    oc = put(A.at[:, col(4)], xo.at[ds(mine, R, R), :], CN)
    ol0 = load(A.at[:, col(0)], xo.at[ds(mine, R, R), :])
    oy.wait_recv()
    r0 = ds(quarter(1 - iy, ic) + z * Z, Z, Z)
    ozy = put(xo.at[r0, :], xo.at[r0, :], ZN)
    oyc.wait_recv()
    r1 = ds(quarter(1 - iy, 1 - ic) + z * Z, Z, Z)
    ozc = put(xo.at[r1, :], xo.at[r1, :], ZN)
    qkv_chunk(2)
    qkv_chunk(3)

    for i in range(4):
        qxr[i].wait_recv()
        ref = at(orows(iy, ic, i), ocol)
        if i % 2 == 0:
            qdr[i] = put(ref, ref, YN)
        qcr.append(put(ref, ref, CN))
        qyr[i].wait_recv()
        ref = at(orows(1 - iy, ic, i), xcol)
        if i % 2 == 1:
            qdr[i] = put(ref, ref, XN)
        qcr.append(put(ref, ref, CN))
    for i in range(4):
        qdr[i].wait_recv()
        ref = at(orows(1 - iy, ic, i), ocol)
        qcr.append(put(ref, ref, CN))
    for c in (oc, ozy, ozc):
        c.wait_recv()
    ol0.wait()
    for i in range(4):
        qown[i].wait()
    for c in qcr:
        c.wait_recv()
    settle(list(sends))


def solution(mesh):
    def body(x, g1, g2, w_gate, w_up, w_down, o, w_o, w_qkv):
        g = jnp.concatenate([g1[None], g2[None], jnp.zeros((6, B), F32)], 0)
        hbm = pl.BlockSpec(memory_space=pl.ANY)
        outs = pl.pallas_call(
            _kernel,
            out_shape=(jax.ShapeDtypeStruct((T, B), BF), jax.ShapeDtypeStruct((T, Q // 2), BF),
                       jax.ShapeDtypeStruct((3, K2, B), BF), jax.ShapeDtypeStruct((8, B, QC), BF)),
            in_specs=[hbm, pl.BlockSpec(memory_space=pltpu.VMEM)] + [hbm] * 6,
            out_specs=(hbm,) * 4,
            scratch_shapes=[
                pltpu.VMEM((R, D), BF), pltpu.VMEM((R, D), BF), pltpu.VMEM((PIECES * D, 2 * PC), BF),
                pltpu.VMEM((R, K2), BF), pltpu.VMEM((Z, 12 * S), F32), pltpu.VMEM((Z, 12 * S), F32),
                pltpu.VMEM((Z, 12 * S), F32), pltpu.VMEM((8, D), F32),
                pltpu.SemaphoreType.DMA((NREMOTE,)), pltpu.SemaphoreType.DMA((NREMOTE,)),
                pltpu.SemaphoreType.DMA((NLOCAL,)),
            ],
            compiler_params=pltpu.CompilerParams(collective_id=0, has_side_effects=True,
                                                 vmem_limit_bytes=67043328),
        )(x, g, w_gate, w_up, w_down, o, w_o, w_qkv)
        return outs[0], outs[1]

    in_specs = (P(None, 'h'), P('h'), P('h'), P('h', 'f'), P('h', 'f'), P('f', 'h'),
                P(None, 'f'), P('f', 'h'), P('h', 'f'))
    return jax.shard_map(body, mesh=mesh, in_specs=in_specs,
                         out_specs=(P(None, 'h'), P(None, 'f')), check_vma=False)
```

```python
import jax
import jax.numpy as jnp
from jax import lax
from jax.experimental import pallas as pl
from jax.experimental.pallas import tpu as pltpu
from jax.sharding import PartitionSpec as P

EPS = 1e-6
BF, F32 = jnp.bfloat16, jnp.float32
MESH = pl.DeviceIdType.MESH
NREMOTE, NLOCAL = 288, 128

T, D, FF, HD, Q = 4096, 3072, 8192, 3072, 5120
B = D // 8
R = T // 4
Z = R // 2
FP = FF // 2
PIECES = 4
PC = FP // 2 // PIECES
K2 = FP + HD // 2
S = 128
QC = Q // 4
QT = 256
QG = ((0, 1), (1, 2), (3, 2))
XFIRST = (2, 5, 8)


def _dot(a, b):
    return jnp.dot(a, b, preferred_element_type=F32)


def _kernel(x, g, wg, wu, wd, o, wo, wq, xo, qo, dl, ql,
            A, N, W, act, ys, yr, yo, gv, send, recv, loc):
    h = lax.axis_index('h')
    z = lax.axis_index('f')
    iy, ix, ic = lax.div(h, 4), lax.rem(lax.div(h, 2), 2), lax.rem(h, 2)

    def dev(kx, ky, kc):
        py = 1 - iy if ky else iy
        px = 1 - ix if kx else ix
        pc = 1 - ic if kc else ic
        return {'h': py * 4 + px * 2 + pc}

    XN, YN, CN, YCN, ZN = dev(1, 0, 0), dev(0, 1, 0), dev(0, 0, 1), dev(0, 1, 1), {'f': 1 - z}
    count = [0, 0]
    sends = []

    def put(src, dst, to):
        i = count[0]
        count[0] += 1
        c = pltpu.make_async_remote_copy(src, dst, send.at[i], recv.at[i], device_id=to, device_id_type=MESH)
        c.start()
        sends.append(c)
        return c

    def load(src, dst):
        i = count[1]
        count[1] += 1
        c = pltpu.make_async_copy(src, dst, loc.at[i])
        c.start()
        return c

    def settle(cs):
        for c in cs:
            c.wait_send()
            sends[:] = [d for d in sends if d is not c]

    def al(v, m):
        return pl.multiple_of(v, m)

    def ds(start, size, m):
        return pl.ds(al(start, m), size)

    def quarter(py, pc):
        return pc * (2 * R) + py * R

    mine = quarter(iy, ic)
    zr = ds(z * Z, Z, Z)
    zo = ds((1 - z) * Z, Z, Z)

    bar = pltpu.get_barrier_semaphore()
    for k in range(1, 8):
        pl.semaphore_signal(bar, inc=1, device_id=dev(k & 1, (k >> 1) & 1, k >> 2), device_id_type=MESH)
    pl.semaphore_signal(bar, inc=1, device_id=ZN, device_id_type=MESH)
    pl.semaphore_wait(bar, 8)

    def col(p):
        return pl.ds(p * B, B)

    x4 = put(x.at[ds(quarter(iy, 1 - ic), R, R), :], A.at[:, col(4)], CN)
    x2 = put(x.at[ds(quarter(1 - iy, ic) + z * Z, Z, Z), :], A.at[zr, col(2)], YN)
    x6 = put(x.at[ds(quarter(1 - iy, 1 - ic) + z * Z, Z, Z), :], A.at[zr, col(6)], YCN)
    x1 = put(x.at[ds(mine + z * Z, Z, Z), :], A.at[zr, col(1)], XN)
    x0 = load(x.at[ds(mine, R, R), :], A.at[:, col(0)])

    def wrow(j, a, n):
        return pl.ds(j * D + a, n)

    wl, wx, wyo, wyf, wc = {}, {}, {}, {}, {}

    def w_load(j):
        c0 = ds(ix * (FP // 2) + j * PC, PC, PC)
        wl[j] = [load(wg.at[:, c0], W.at[wrow(j, 0, B), pl.ds(0, PC)]),
                 load(wu.at[:, c0], W.at[wrow(j, 0, B), pl.ds(PC, PC)])]

    def w_x(j):
        c1 = ds((1 - ix) * (FP // 2) + j * PC, PC, PC)
        wx[j] = [put(wg.at[:, c1], W.at[wrow(j, B, B), pl.ds(0, PC)], XN),
                 put(wu.at[:, c1], W.at[wrow(j, B, B), pl.ds(PC, PC)], XN)]

    def w_yown(j):
        for c in wl[j]:
            c.wait()
        wyo[j] = put(W.at[wrow(j, 0, B), :], W.at[wrow(j, 2 * B, B), :], YN)

    def w_xgot(j):
        for c in wx[j]:
            c.wait_recv()
        wyf[j] = put(W.at[wrow(j, B, B), :], W.at[wrow(j, 3 * B, B), :], YN)
        wc[j] = [put(W.at[wrow(j, 0, 2 * B), :], W.at[wrow(j, 4 * B, 2 * B), :], CN)]

    def w_ygot(j):
        wyo[j].wait_recv()
        wc[j].append(put(W.at[wrow(j, 2 * B, B), :], W.at[wrow(j, 6 * B, B), :], CN))
        wyf[j].wait_recv()
        wc[j].append(put(W.at[wrow(j, 3 * B, B), :], W.at[wrow(j, 7 * B, B), :], CN))

    for j in range(PIECES):
        w_load(j)
    w_x(0)
    gs = [put(g, gv.at[:, col(k)], dev(k & 1, (k >> 1) & 1, k >> 2)) for k in range(1, 8)]
    g0 = load(g, gv.at[:, col(0)])
    w_yown(0)
    w_yown(1)
    ol = load(o.at[ds(mine, R, R), :], act.at[:, pl.ds(FP, HD // 2)])

    dc = [put(wd, dl.at[1, pl.ds(0, FP), :], CN), put(wo, dl.at[1, pl.ds(FP, HD // 2), :], CN)]
    qc0 = put(wq.at[:, ds(ix * QC, QC, QC)], ql.at[4], CN)

    x4.wait_recv()
    x5 = put(A.at[zr, col(4)], A.at[zr, col(5)], XN)
    zs = []

    def zput(p):
        zs.append(put(A.at[zr, col(p)], A.at[zr, col(p)], ZN))

    x1.wait_recv()
    zput(1)
    x2.wait_recv()
    x3 = put(A.at[zr, col(2)], A.at[zr, col(3)], XN)
    zput(2)
    x6.wait_recv()
    x7 = put(A.at[zr, col(6)], A.at[zr, col(7)], XN)
    zput(6)
    for j in range(1, PIECES):
        w_x(j)
    w_xgot(0)
    w_yown(2)
    x5.wait_recv()
    zput(5)
    x3.wait_recv()
    zput(3)
    x7.wait_recv()
    zput(7)
    for c in gs:
        c.wait_recv()
    g0.wait()
    x0.wait()
    for c in zs:
        c.wait_recv()

    def norm(row, n, gi):
        gain = gv[gi:gi + 1, :]

        def body(i, _):
            rows = ds(row + i * 32, 32, 32)
            v = A[rows, :].astype(F32)
            ss = jnp.sum(v * v, axis=-1, keepdims=True)
            N[rows, :] = (v * lax.rsqrt(ss / D + EPS) * gain).astype(BF)
            return 0

        lax.fori_loop(0, n // 32, body, 0)

    norm(0, R, 0)

    def gate_up(j, half):
        def body(t, _):
            rows = ds(half * Z + lax.div(t, 2) * 256, 256, 256)
            c = lax.rem(t, 2) * 256
            n = N[rows, :]
            gt = _dot(n, W[wrow(j, 0, D), ds(c, 256, 256)])
            up = _dot(n, W[wrow(j, 0, D), ds(PC + c, 256, 256)])
            act[rows, ds(j * PC + c, 256, 256)] = (jax.nn.silu(gt) * up).astype(BF)
            return 0

        lax.fori_loop(0, (Z // 256) * (PC // 256), body, 0)

    dy, dyc, dloads = {}, {}, {}

    def down_y(p):
        c = pl.ds(p * S, S)
        dy[p] = [put(wd.at[:, c], dl.at[0, pl.ds(0, FP), c], YN),
                 put(wo.at[:, c], dl.at[0, pl.ds(FP, HD // 2), c], YN)]

    def down_load(ky, p):
        out = []
        for kc in range(2):
            c = pl.ds(p * S, S)
            if ky == 0 and kc == 0:
                top, bot = wd, wo.at[:, c]
            else:
                k = {(1, 0): 0, (0, 1): 1, (1, 1): 2}[ky, kc]
                top, bot = dl.at[k], dl.at[k, pl.ds(FP, HD // 2), c]
            to = pl.ds(p * 2 * S + kc * S, S)
            r0 = ky * K2
            out.append(load(top.at[ds(ix * (FP // 2), FP // 2, FP // 2), c], W.at[pl.ds(r0, FP // 2), to]))
            out.append(load(top.at[ds((1 - ix) * (FP // 2), FP // 2, FP // 2), c], W.at[pl.ds(r0 + FP // 2, FP // 2), to]))
            out.append(load(bot, W.at[pl.ds(r0 + FP, HD // 2), to]))
        dloads[ky, p] = out

    def w_settle(j):
        settle(wx[j] + [wyo[j], wyf[j]] + wc[j])

    acts = {}

    def act_put(j, half):
        rows = zo if half else zr
        acts[j, half] = put(act.at[rows, pl.ds(j * PC, PC)], act.at[rows, pl.ds(FP // 2 + j * PC, PC)], XN)

    for j in range(PIECES):
        if j + 1 < PIECES:
            w_xgot(j + 1)
        if j == 0:
            w_yown(3)
        if j == 2:
            for p in range(3):
                down_y(p)
        if j == 3:
            w_settle(0)
            w_settle(1)
            for c in dc:
                c.wait_recv()
            for p in range(3):
                down_load(0, p)
        w_ygot(j)
        for c in wc[j]:
            c.wait_recv()
        gate_up(j, 1 - z)
        if j == 0:
            settle(zs + [x1, x2, x3, x4, x5, x6, x7] + gs)
        act_put(j, 1)
        if j == 3:
            act_put(2, 0)
        gate_up(j, z)
        if j != 2:
            act_put(j, 0)

    qx = put(wq.at[:, ds((1 - ix) * QC, QC, QC)], ql.at[1], XN)
    w_settle(2)
    w_settle(3)

    rs = {}

    def step(ky, p):
        return (ky * 3 + p) * 2 * S

    def down(ky, p, half, dst):
        def f(i, _):
            w = W[pl.ds(ky * K2, K2), pl.ds(p * 2 * S, 2 * S)]
            dst[ds(i * 256, 256, 256), pl.ds(step(ky, p), 2 * S)] = _dot(act[ds(half * Z + i * 256, 256, 256), :], w)
            return 0
        lax.fori_loop(0, Z // 256, f, 0)

    def down_far(ky, p):
        for c in dloads[ky, p]:
            c.wait()
        down(ky, p, 1 - z, ys)
        s = pl.ds(step(ky, p), 2 * S)
        rs[ky, p] = put(ys.at[:, s], yr.at[:, s], ZN)

    def down_near(ky, p):
        down(ky, p, z, yo)

    def acol(ky, p, kc, kx=0):
        return pl.ds((2 * ky + 4 * kc + kx) * B + p * S, S)

    xx, xz, xf = {}, {}, {}

    def finish(ky, p):
        rs[ky, p].wait_recv()

        def f(i, _):
            r = ds(i * 64, 64, 64)
            ra = ds(z * Z + i * 64, 64, 64)
            for kc in range(2):
                s = pl.ds(step(ky, p) + kc * S, S)
                c = acol(ky, p, kc)
                A[ra, c] = (A[ra, c].astype(F32) + (yo[r, s] + yr[r, s])).astype(BF)
            return 0

        lax.fori_loop(0, Z // 64, f, 0)
        for kc in range(2):
            xx[ky, p, kc] = put(A.at[zr, acol(ky, p, kc)], A.at[zr, acol(ky, p, kc, 1)], XN)

    def z_own(ky, p):
        for kc in range(2):
            c = acol(ky, p, kc)
            xz[ky, p, kc] = put(A.at[zr, c], A.at[zr, c], ZN)

    def x_got(ky, p):
        for kc in range(2):
            xx[ky, p, kc].wait_recv()

    def z_far(ky, p):
        for kc in range(2):
            c = acol(ky, p, kc, 1)
            xf[ky, p, kc] = put(A.at[zr, c], A.at[zr, c], ZN)

    def down_ygot(p):
        for c in dy[p]:
            c.wait_recv()
        c = pl.ds(p * S, S)
        dyc[p] = put(dl.at[0, :, c], dl.at[2, :, c], CN)

    def down_ready(p):
        dyc[p].wait_recv()
        down_load(1, p)

    ol.wait()
    for j in range(PIECES):
        acts[j, 1].wait_recv()
    for p in range(3):
        down_far(0, p)
    down_ygot(0)
    down_ready(0)
    down_far(1, 0)
    for j in range(PIECES):
        acts[j, 0].wait_recv()
    for p in range(3):
        down_near(0, p)
    finish(0, 0)
    finish(0, 1)
    down_near(1, 0)
    finish(0, 2)

    qyo, qyf, qcy, qloads = {}, {}, {}, {}

    def tile(t, n=1):
        return pl.ds(t * QT, n * QT)

    def qw_y(gi):
        t, n = QG[gi]
        qyo[gi] = put(wq.at[:, ds(ix * QC + t * QT, n * QT, QT)], ql.at[2, :, tile(t, n)], YN)
        qyf[gi] = put(ql.at[1, :, tile(t, n)], ql.at[3, :, tile(t, n)], YN)

    def qw_ygot(gi):
        t, n = QG[gi]
        qyo[gi].wait_recv()
        a1 = put(ql.at[2, :, tile(t, n)], ql.at[6, :, tile(t, n)], CN)
        qyf[gi].wait_recv()
        a2 = put(ql.at[3, :, tile(t, n)], ql.at[7, :, tile(t, n)], CN)
        qcy[gi] = (a1, a2)

    def slot(t, k):
        return W.at[pl.ds((D if t == 4 else 0) + k * B, B), pl.ds(3 * QT if t == 4 else t * QT, QT)]

    def qload(gi, ks):
        t0, n = QG[gi]
        for t in range(t0, t0 + n):
            for k in ks:
                src = wq.at[:, ds(ix * QC + t * QT, QT, QT)] if k == 0 else ql.at[k, :, tile(t)]
                qloads.setdefault(t, []).append(load(src, slot(t, k)))

    qx.wait_recv()
    qc1 = put(ql.at[1], ql.at[5], CN)
    for gi in range(len(QG)):
        qw_y(gi)
    qc0.wait_recv()
    qc1.wait_recv()
    for gi in range(len(QG)):
        qload(gi, (0, 1, 4, 5))

    down_ygot(1)
    down_ready(1)
    down_far(1, 1)
    for p in range(3):
        z_own(0, p)
    finish(1, 0)
    down_near(1, 1)
    for p in range(3):
        x_got(0, p)
    finish(1, 1)
    down_ygot(2)
    down_ready(2)
    down_far(1, 2)
    for p in range(3):
        z_far(0, p)
    for p in range(2):
        z_own(1, p)
    for p in range(2):
        x_got(1, p)
        z_far(1, p)
    down_near(1, 2)
    settle([acts[k] for k in acts])
    qw_ygot(0)
    finish(1, 2)
    z_own(1, 2)
    for c in qcy[0]:
        c.wait_recv()
    qload(0, (2, 3, 6, 7))
    x_got(1, 2)
    z_far(1, 2)
    norm(z * Z, Z, 1)

    qxr, qyr, qdr, qcr, qown = {}, {}, {}, [], []

    def at(u, fy, fx):
        half, t = (z if u < 5 else 1 - z), u % 5
        py = 1 - iy if fy else iy
        px = 1 - ix if fx else ix
        return qo.at[ds(quarter(py, ic) + half * Z, Z, Z), ds(px * QC + t * QT, QT, QT)]

    def unit(u):
        t = u % 5
        if u < 5:
            for c in qloads[t]:
                c.wait()
        half = z if u < 5 else 1 - z

        def f(i, _):
            rows = ds(half * Z + i * 256, 256, 256)
            w = W[pl.ds(D if t == 4 else 0, D), pl.ds(3 * QT if t == 4 else t * QT, QT)]
            act[rows, pl.ds(t * QT, QT)] = _dot(N[rows, :], w).astype(BF)
            return 0

        lax.fori_loop(0, Z // 256, f, 0)
        src, dst = act.at[ds(half * Z, Z, Z), pl.ds(t * QT, QT)], at(u, 0, 0)
        qxr[u] = put(src, dst, XN)
        qyr[u] = put(src, dst, YN)
        qcr.append(put(src, dst, CN))
        qown.append(load(src, dst))

    def got_x(u):
        qxr[u].wait_recv()
        ref = at(u, 0, 1)
        if u in XFIRST:
            qdr[u] = put(ref, ref, YN)
        qcr.append(put(ref, ref, CN))

    def got_y(u):
        qyr[u].wait_recv()
        ref = at(u, 1, 0)
        if u not in XFIRST:
            qdr[u] = put(ref, ref, XN)
        qcr.append(put(ref, ref, CN))

    def got_d(u):
        qdr[u].wait_recv()
        ref = at(u, 1, 1)
        qcr.append(put(ref, ref, CN))

    unit(0)
    qw_ygot(1)
    for c in qcy[1]:
        c.wait_recv()
    qload(1, (2, 3, 6, 7))
    unit(1)
    unit(2)
    got_x(0)
    qw_ygot(2)
    for c in qcy[2]:
        c.wait_recv()
    qload(2, (2, 3, 6, 7))
    unit(3)
    unit(4)
    orow = ds(mine + z * Z, Z, Z)
    oy = put(A.at[zr, col(2)], xo.at[orow, :], YN)
    oyc = put(A.at[zr, col(6)], xo.at[orow, :], YCN)
    got_y(0)
    got_x(1)
    got_y(1)
    got_x(2)
    got_y(2)
    for k in xz:
        xz[k].wait_recv()
    for k in xf:
        xf[k].wait_recv()
    norm((1 - z) * Z, Z, 1)
    unit(5)
    unit(6)
    got_x(3)
    got_y(3)
    unit(7)
    unit(8)
    got_x(4)
    got_y(4)
    unit(9)
    oc = put(A.at[:, col(4)], xo.at[ds(mine, R, R), :], CN)
    ol0 = load(A.at[:, col(0)], xo.at[ds(mine, R, R), :])
    oy.wait_recv()
    r0 = ds(quarter(1 - iy, ic) + z * Z, Z, Z)
    ozy = put(xo.at[r0, :], xo.at[r0, :], ZN)
    oyc.wait_recv()
    r1 = ds(quarter(1 - iy, 1 - ic) + z * Z, Z, Z)
    ozc = put(xo.at[r1, :], xo.at[r1, :], ZN)
    for u in range(5, 10):
        got_x(u)
        got_y(u)
        got_d(u - 5)
    for u in range(5, 10):
        got_d(u)
    for c in (oc, ozy, ozc):
        c.wait_recv()
    ol0.wait()
    for c in qown:
        c.wait()
    for c in qcr:
        c.wait_recv()
    settle(list(sends))


def _copy(a, b, ao, bo):
    ao[...] = a[...]
    bo[...] = b[...]


def _hand_over(a, b, rows=512):
    spec = lambda v: pl.BlockSpec((rows, v.shape[1]), lambda i: (i, 0))
    return pl.pallas_call(
        _copy,
        grid=(a.shape[0] // rows,),
        out_shape=(jax.ShapeDtypeStruct(a.shape, a.dtype), jax.ShapeDtypeStruct(b.shape, b.dtype)),
        in_specs=[spec(a), spec(b)],
        out_specs=(spec(a), spec(b)),
    )(a, b)


def solution(mesh):
    def body(x, g1, g2, w_gate, w_up, w_down, o, w_o, w_qkv):
        g = jnp.concatenate([g1[None], g2[None], jnp.zeros((6, B), F32)], 0)
        hbm = pl.BlockSpec(memory_space=pl.ANY)
        outs = pl.pallas_call(
            _kernel,
            out_shape=(jax.ShapeDtypeStruct((T, B), BF), jax.ShapeDtypeStruct((T, Q // 2), BF),
                       jax.ShapeDtypeStruct((3, K2, B), BF), jax.ShapeDtypeStruct((8, B, QC), BF)),
            in_specs=[hbm, pl.BlockSpec(memory_space=pltpu.VMEM)] + [hbm] * 6,
            out_specs=(hbm,) * 4,
            scratch_shapes=[
                pltpu.VMEM((R, D), BF), pltpu.VMEM((R, D), BF), pltpu.VMEM((PIECES * D, 2 * PC), BF),
                pltpu.VMEM((R, K2), BF), pltpu.VMEM((Z, 12 * S), F32), pltpu.VMEM((Z, 12 * S), F32),
                pltpu.VMEM((Z, 12 * S), F32), pltpu.VMEM((8, D), F32),
                pltpu.SemaphoreType.DMA((NREMOTE,)), pltpu.SemaphoreType.DMA((NREMOTE,)),
                pltpu.SemaphoreType.DMA((NLOCAL,)),
            ],
            compiler_params=pltpu.CompilerParams(collective_id=0, has_side_effects=True,
                                                 vmem_limit_bytes=67043328),
        )(x, g, w_gate, w_up, w_down, o, w_o, w_qkv)
        return _hand_over(outs[0], outs[1])

    in_specs = (P(None, 'h'), P('h'), P('h'), P('h', 'f'), P('h', 'f'), P('f', 'h'),
                P(None, 'f'), P('f', 'h'), P('h', 'f'))
    return jax.shard_map(body, mesh=mesh, in_specs=in_specs,
                         out_specs=(P(None, 'h'), P(None, 'f')), check_vma=False)
```

```python
import jax
import jax.numpy as jnp
from jax import lax
from jax.experimental import pallas as pl
from jax.experimental.pallas import tpu as pltpu
from jax.sharding import PartitionSpec as P

EPS = 1e-6
BF, F32 = jnp.bfloat16, jnp.float32
MESH = pl.DeviceIdType.MESH
NREMOTE, NLOCAL = 288, 128

T, D, FF, HD, Q = 4096, 3072, 8192, 3072, 5120
B = D // 8
R = T // 4
Z = R // 2
FP = FF // 2
PIECES = 4
PC = FP // 2 // PIECES
K2 = FP + HD // 2
S = 128
QC = Q // 4
QT = 256
QG = ((0, 1), (1, 2), (3, 2))
QSLOT = ((0, 512), (D, 512), (0, 768), (D, 768), (0, 0))
VMEM_LIMIT = 67043328 - T * (B + Q // 2) * 2 - 65536
XFIRST = (2, 5, 8)


def _dot(a, b):
    return jnp.dot(a, b, preferred_element_type=F32)


def _kernel(x, g, wg, wu, wd, o, wo, wq, xo, qo, dl, ql, wh,
            A, N, W, act, ys, yr, yo, gv, send, recv, loc):
    h = lax.axis_index('h')
    z = lax.axis_index('f')
    iy, ix, ic = lax.div(h, 4), lax.rem(lax.div(h, 2), 2), lax.rem(h, 2)

    def dev(kx, ky, kc):
        py = 1 - iy if ky else iy
        px = 1 - ix if kx else ix
        pc = 1 - ic if kc else ic
        return {'h': py * 4 + px * 2 + pc}

    XN, YN, CN, YCN, ZN = dev(1, 0, 0), dev(0, 1, 0), dev(0, 0, 1), dev(0, 1, 1), {'f': 1 - z}
    count = [0, 0]
    sends = []

    def put(src, dst, to):
        i = count[0]
        count[0] += 1
        c = pltpu.make_async_remote_copy(src, dst, send.at[i], recv.at[i], device_id=to, device_id_type=MESH)
        c.start()
        sends.append(c)
        return c

    def load(src, dst):
        i = count[1]
        count[1] += 1
        c = pltpu.make_async_copy(src, dst, loc.at[i])
        c.start()
        return c

    def settle(cs):
        for c in cs:
            c.wait_send()
            sends[:] = [d for d in sends if d is not c]

    def al(v, m):
        return pl.multiple_of(v, m)

    def ds(start, size, m):
        return pl.ds(al(start, m), size)

    def quarter(py, pc):
        return pc * (2 * R) + py * R

    mine = quarter(iy, ic)
    zr = ds(z * Z, Z, Z)
    zo = ds((1 - z) * Z, Z, Z)

    bar = pltpu.get_barrier_semaphore()
    for k in range(1, 8):
        pl.semaphore_signal(bar, inc=1, device_id=dev(k & 1, (k >> 1) & 1, k >> 2), device_id_type=MESH)
    pl.semaphore_signal(bar, inc=1, device_id=ZN, device_id_type=MESH)
    pl.semaphore_wait(bar, 8)

    def col(p):
        return pl.ds(p * B, B)

    x4 = put(x.at[ds(quarter(iy, 1 - ic), R, R), :], A.at[:, col(4)], CN)
    x2 = put(x.at[ds(quarter(1 - iy, ic) + z * Z, Z, Z), :], A.at[zr, col(2)], YN)
    x6 = put(x.at[ds(quarter(1 - iy, 1 - ic) + z * Z, Z, Z), :], A.at[zr, col(6)], YCN)
    x1 = put(x.at[ds(mine + z * Z, Z, Z), :], A.at[zr, col(1)], XN)
    x0 = load(x.at[ds(mine, R, R), :], A.at[:, col(0)])

    def wrow(j, a, n):
        return pl.ds((j % 2) * D + a, n)

    def wref(j, a, n, c=slice(None)):
        return W.at[wrow(j, a, n), c] if j < 2 else wh.at[j - 2, pl.ds(a, n), c]

    wl, wx, wyo, wyf, wc = {}, {}, {}, {}, {}
    GC, UC = pl.ds(0, PC), pl.ds(PC, PC)

    def wcol(j, other):
        return ds(((1 - ix) if other else ix) * (FP // 2) + j * PC, PC, PC)

    def w_load(j):
        c0 = wcol(j, 0)
        wl[j] = [load(wg.at[:, c0], W.at[wrow(j, 0, B), GC]), load(wu.at[:, c0], W.at[wrow(j, 0, B), UC])]

    def w_x(j):
        c1 = wcol(j, 1)
        wx[j] = [put(wg.at[:, c1], wref(j, B, B, GC), XN), put(wu.at[:, c1], wref(j, B, B, UC), XN)]

    def w_yown(j):
        if j < 2:
            for c in wl[j]:
                c.wait()
            wyo[j] = [put(wref(j, 0, B), wref(j, 2 * B, B), YN)]
            wc[j] = [put(wref(j, 0, B), wref(j, 4 * B, B), CN)]
        else:
            c0 = wcol(j, 0)
            wyo[j] = [put(wg.at[:, c0], wref(j, 2 * B, B, GC), YN), put(wu.at[:, c0], wref(j, 2 * B, B, UC), YN)]
            wc[j] = [put(wg.at[:, c0], wref(j, 4 * B, B, GC), CN), put(wu.at[:, c0], wref(j, 4 * B, B, UC), CN)]

    def w_xgot(j):
        for c in wx[j]:
            c.wait_recv()
        wyf[j] = [put(wref(j, B, B), wref(j, 3 * B, B), YN)]
        wc[j].append(put(wref(j, B, B), wref(j, 5 * B, B), CN))

    def w_block(j, k, n=1):
        return load(wref(j, k * B, n * B), W.at[wrow(j, k * B, n * B), :])

    def w_ygot(j):
        for c in wyo[j]:
            c.wait_recv()
        own = len(wc[j])
        wc[j].append(put(wref(j, 2 * B, B), wref(j, 6 * B, B), CN))
        loads = []
        if j >= 2:
            w_load(j)
            for c in wc[j][:own]:
                c.wait_recv()
            loads = wl[j] + [w_block(j, 1, 2), w_block(j, 4, 2)]
        for c in wyf[j]:
            c.wait_recv()
        wc[j].append(put(wref(j, 3 * B, B), wref(j, 7 * B, B), CN))
        if j >= 2:
            loads.append(w_block(j, 3))
        for c in wc[j] if j < 2 else wc[j][own:]:
            c.wait_recv()
        if j >= 2:
            loads.append(w_block(j, 6, 2))
        for c in loads:
            c.wait()

    w_load(0)
    w_load(1)
    w_x(0)
    gs = [put(g, gv.at[:, col(k)], dev(k & 1, (k >> 1) & 1, k >> 2)) for k in range(1, 8)]
    g0 = load(g, gv.at[:, col(0)])
    w_yown(0)
    w_yown(1)

    dc = [put(wd, dl.at[1, pl.ds(0, FP), :], CN), put(wo, dl.at[1, pl.ds(FP, HD // 2), :], CN)]
    qc0 = put(wq.at[:, ds(ix * QC, QC, QC)], ql.at[4], CN)

    x4.wait_recv()
    x5 = put(A.at[zr, col(4)], A.at[zr, col(5)], XN)
    zs = []

    def zput(p):
        zs.append(put(A.at[zr, col(p)], A.at[zr, col(p)], ZN))

    x1.wait_recv()
    zput(1)
    x2.wait_recv()
    x3 = put(A.at[zr, col(2)], A.at[zr, col(3)], XN)
    zput(2)
    x6.wait_recv()
    x7 = put(A.at[zr, col(6)], A.at[zr, col(7)], XN)
    zput(6)
    for j in range(1, PIECES):
        w_x(j)
    w_xgot(0)
    w_yown(2)
    x5.wait_recv()
    zput(5)
    x3.wait_recv()
    zput(3)
    x7.wait_recv()
    zput(7)
    for c in gs:
        c.wait_recv()
    g0.wait()
    x0.wait()
    for c in zs:
        c.wait_recv()

    def norm(row, n, gi):
        gain = gv[gi:gi + 1, :]

        def body(i, _):
            rows = ds(row + i * 32, 32, 32)
            v = A[rows, :].astype(F32)
            ss = jnp.sum(v * v, axis=-1, keepdims=True)
            N[rows, :] = (v * lax.rsqrt(ss / D + EPS) * gain).astype(BF)
            return 0

        lax.fori_loop(0, n // 32, body, 0)

    norm(0, R, 0)

    def gate_up(j, half):
        def body(t, _):
            rows = ds(half * Z + lax.div(t, 2) * 256, 256, 256)
            c = lax.rem(t, 2) * 256
            n = N[rows, :]
            gt = _dot(n, W[wrow(j, 0, D), ds(c, 256, 256)])
            up = _dot(n, W[wrow(j, 0, D), ds(PC + c, 256, 256)])
            act[rows, ds(j * PC + c, 256, 256)] = (jax.nn.silu(gt) * up).astype(BF)
            return 0

        lax.fori_loop(0, (Z // 256) * (PC // 256), body, 0)

    dy, dyc, dloads = {}, {}, {}

    def down_y(p):
        c = pl.ds(p * S, S)
        dy[p] = [put(wd.at[:, c], dl.at[0, pl.ds(0, FP), c], YN),
                 put(wo.at[:, c], dl.at[0, pl.ds(FP, HD // 2), c], YN)]

    def dslot(ky, p):
        return ((ky * 3 + p) % 4) * 2 * S

    def down_load(ky, p):
        out = []
        for kc in range(2):
            c = pl.ds(p * S, S)
            if ky == 0 and kc == 0:
                top, bot = wd, wo.at[:, c]
            else:
                k = {(1, 0): 0, (0, 1): 1, (1, 1): 2}[ky, kc]
                top, bot = dl.at[k], dl.at[k, pl.ds(FP, HD // 2), c]
            to = pl.ds(dslot(ky, p) + kc * S, S)
            out.append(load(top.at[ds(ix * (FP // 2), FP // 2, FP // 2), c], W.at[pl.ds(0, FP // 2), to]))
            out.append(load(top.at[ds((1 - ix) * (FP // 2), FP // 2, FP // 2), c], W.at[pl.ds(FP // 2, FP // 2), to]))
            out.append(load(bot, W.at[pl.ds(FP, HD // 2), to]))
        dloads[ky, p] = out

    def w_settle(j):
        settle(wx[j] + wyo[j] + wyf[j] + wc[j])

    acts = {}

    def act_put(j, half):
        rows = zo if half else zr
        acts[j, half] = put(act.at[rows, pl.ds(j * PC, PC)], act.at[rows, pl.ds(FP // 2 + j * PC, PC)], XN)

    for j in range(PIECES):
        if j + 1 < PIECES:
            w_xgot(j + 1)
        if j == 0:
            w_yown(3)
        if j == 2:
            w_settle(0)
            for p in range(3):
                down_y(p)
        if j == 3:
            w_settle(1)
        w_ygot(j)
        gate_up(j, 1 - z)
        if j == 0:
            settle(zs + [x1, x2, x3, x4, x5, x6, x7] + gs)
        act_put(j, 1)
        if j == 3:
            act_put(2, 0)
        gate_up(j, z)
        if j != 2:
            act_put(j, 0)

    qx = put(wq.at[:, ds((1 - ix) * QC, QC, QC)], ql.at[1], XN)
    for c in dc:
        c.wait_recv()
    for p in range(3):
        down_load(0, p)
    ol = load(o.at[ds(mine, R, R), :], N.at[:, pl.ds(0, HD // 2)])

    rs = {}

    def step(ky, p):
        return (ky * 3 + p) * 2 * S

    def down(ky, p, half, dst, at, i0=0, n=Z // 256):
        def f(i, _):
            c = pl.ds(dslot(ky, p), 2 * S)
            rows = ds(half * Z + i * 256, 256, 256)
            dst[ds(i * 256, 256, 256), pl.ds(at, 2 * S)] = (
                _dot(act[rows, :], W[pl.ds(0, FP), c]) + _dot(N[rows, pl.ds(0, HD // 2)], W[pl.ds(FP, HD // 2), c]))
            return 0
        lax.fori_loop(i0, i0 + n, f, 0)

    def parts(ky, p):
        return ((0, 256), (256, 256)) if (ky, p) == (1, 2) else ((0, Z),)

    def down_far(ky, p):
        for c in dloads[ky, p]:
            c.wait()
        s = pl.ds(step(ky, p), 2 * S)
        for r, n in parts(ky, p):
            down(ky, p, 1 - z, ys, step(ky, p), r // 256, n // 256)
            rs[ky, p, r] = put(ys.at[pl.ds(r, n), s], yr.at[pl.ds(r, n), s], ZN)

    def near(ky, p):
        return ((ky * 3 + p) % 2) * 2 * S

    def down_near(ky, p):
        down(ky, p, z, yo, near(ky, p))

    def acol(ky, p, kc, kx=0):
        return pl.ds((2 * ky + 4 * kc + kx) * B + p * S, S)

    xx, xz, xf = {}, {}, {}

    def finish(ky, p):
        for r0, n in parts(ky, p):
            rs[ky, p, r0].wait_recv()

            def f(i, _):
                r = ds(r0 + i * 64, 64, 64)
                ra = ds(z * Z + r0 + i * 64, 64, 64)
                for kc in range(2):
                    c = acol(ky, p, kc)
                    mine_y = yo[r, pl.ds(near(ky, p) + kc * S, S)]
                    A[ra, c] = (A[ra, c].astype(F32) + (mine_y + yr[r, pl.ds(step(ky, p) + kc * S, S)])).astype(BF)
                return 0

            lax.fori_loop(0, n // 64, f, 0)
            rows = ds(z * Z + r0, n, n)
            for kc in range(2):
                xx[ky, p, kc, r0] = put(A.at[rows, acol(ky, p, kc)], A.at[rows, acol(ky, p, kc, 1)], XN)

    def z_own(ky, p):
        for kc in range(2):
            c = acol(ky, p, kc)
            xz[ky, p, kc] = put(A.at[zr, c], A.at[zr, c], ZN)

    def x_got(ky, p):
        for r0, _ in parts(ky, p):
            for kc in range(2):
                xx[ky, p, kc, r0].wait_recv()

    def z_far(ky, p):
        for kc in range(2):
            c = acol(ky, p, kc, 1)
            xf[ky, p, kc] = put(A.at[zr, c], A.at[zr, c], ZN)

    def down_ygot(p):
        for c in dy[p]:
            c.wait_recv()
        c = pl.ds(p * S, S)
        dyc[p] = put(dl.at[0, :, c], dl.at[2, :, c], CN)

    def down_ready(p):
        dyc[p].wait_recv()
        down_load(1, p)

    ol.wait()
    for j in range(PIECES):
        acts[j, 1].wait_recv()
    for p in range(3):
        down_far(0, p)
    down_ygot(0)
    down_ready(0)
    down_far(1, 0)
    for j in range(PIECES):
        acts[j, 0].wait_recv()
    down_near(0, 0)
    down_near(0, 1)
    finish(0, 0)
    down_near(0, 2)
    finish(0, 1)
    down_near(1, 0)
    finish(0, 2)

    qyo, qyf, qcy, qloads = {}, {}, {}, {}

    def tile(t, n=1):
        return pl.ds(t * QT, n * QT)

    def qw_y(gi):
        t, n = QG[gi]
        qyo[gi] = put(wq.at[:, ds(ix * QC + t * QT, n * QT, QT)], ql.at[2, :, tile(t, n)], YN)
        qyf[gi] = put(ql.at[1, :, tile(t, n)], ql.at[3, :, tile(t, n)], YN)

    def qw_ygot(gi):
        t, n = QG[gi]
        qyo[gi].wait_recv()
        a1 = put(ql.at[2, :, tile(t, n)], ql.at[6, :, tile(t, n)], CN)
        qyf[gi].wait_recv()
        a2 = put(ql.at[3, :, tile(t, n)], ql.at[7, :, tile(t, n)], CN)
        qcy[gi] = (a1, a2)

    def slot(t, k):
        r, c = QSLOT[t]
        return W.at[pl.ds(r + k * B, B), pl.ds(c, QT)]

    def qload(gi, ks):
        t0, n = QG[gi]
        for t in range(t0, t0 + n):
            for k in ks:
                src = wq.at[:, ds(ix * QC + t * QT, QT, QT)] if k == 0 else ql.at[k, :, tile(t)]
                qloads.setdefault(t, []).append(load(src, slot(t, k)))

    qx.wait_recv()
    qc1 = put(ql.at[1], ql.at[5], CN)
    for gi in range(len(QG)):
        qw_y(gi)
    qc0.wait_recv()
    qc1.wait_recv()
    for gi in range(2):
        qload(gi, (0, 1, 4, 5))

    down_ygot(1)
    down_ready(1)
    down_far(1, 1)
    for p in range(3):
        z_own(0, p)
    finish(1, 0)
    down_near(1, 1)
    qload(2, (0, 1, 4, 5))
    for p in range(3):
        x_got(0, p)
    finish(1, 1)
    down_ygot(2)
    down_ready(2)
    down_far(1, 2)
    for p in range(3):
        z_far(0, p)
    for p in range(2):
        z_own(1, p)
    for p in range(2):
        x_got(1, p)
        z_far(1, p)
    down_near(1, 2)
    qw_ygot(0)
    finish(1, 2)
    z_own(1, 2)
    for c in qcy[0]:
        c.wait_recv()
    qload(0, (2, 3, 6, 7))
    x_got(1, 2)
    z_far(1, 2)
    norm(z * Z, Z, 1)

    qxr, qyr, qdr, qcr = {}, {}, {}, []

    def at(u, fy, fx):
        half, t = (z if u < 5 else 1 - z), u % 5
        py = 1 - iy if fy else iy
        px = 1 - ix if fx else ix
        return qo.at[ds(quarter(py, ic) + half * Z, Z, Z), ds(px * QC + t * QT, QT, QT)]

    def unit(u):
        t = u % 5
        if u < 5:
            for c in qloads[t]:
                c.wait()
        half = z if u < 5 else 1 - z

        def f(i, _):
            r, c = QSLOT[t]
            w = W[pl.ds(r, D), pl.ds(c, QT)]
            to = qo.at[ds(mine + half * Z + i * 256, 256, 256), ds(ix * QC + t * QT, QT, QT)]
            to[...] = _dot(N[ds(half * Z + i * 256, 256, 256), :], w).astype(BF)
            return 0

        lax.fori_loop(0, Z // 256, f, 0)
        ref = at(u, 0, 0)
        qxr[u] = put(ref, ref, XN)
        qyr[u] = put(ref, ref, YN)
        qcr.append(put(ref, ref, CN))

    def got_x(u):
        qxr[u].wait_recv()
        ref = at(u, 0, 1)
        if u in XFIRST:
            qdr[u] = put(ref, ref, YN)
        qcr.append(put(ref, ref, CN))

    def got_y(u):
        qyr[u].wait_recv()
        ref = at(u, 1, 0)
        if u not in XFIRST:
            qdr[u] = put(ref, ref, XN)
        qcr.append(put(ref, ref, CN))

    def got_d(u):
        qdr[u].wait_recv()
        ref = at(u, 1, 1)
        qcr.append(put(ref, ref, CN))

    unit(0)
    qw_ygot(1)
    for c in qcy[1]:
        c.wait_recv()
    qload(1, (2, 3, 6, 7))
    unit(1)
    unit(2)
    got_x(0)
    qw_ygot(2)
    for c in qcy[2]:
        c.wait_recv()
    qload(2, (2, 3, 6, 7))
    unit(3)
    unit(4)
    orow = ds(mine + z * Z, Z, Z)
    oy = put(A.at[zr, col(2)], xo.at[orow, :], YN)
    oyc = put(A.at[zr, col(6)], xo.at[orow, :], YCN)
    got_y(0)
    got_x(1)
    got_y(1)
    got_x(2)
    got_y(2)
    for k in xz:
        xz[k].wait_recv()
    for k in xf:
        xf[k].wait_recv()
    norm((1 - z) * Z, Z, 1)
    unit(5)
    unit(6)
    got_x(3)
    got_y(3)
    unit(7)
    unit(8)
    got_x(4)
    got_y(4)
    unit(9)
    oc = put(A.at[:, col(4)], xo.at[ds(mine, R, R), :], CN)

    def keep(i, _):
        xo[ds(mine + i * 128, 128, 128), :] = A[ds(i * 128, 128, 128), col(0)]
        return 0

    lax.fori_loop(0, R // 128, keep, 0)
    oy.wait_recv()
    r0 = ds(quarter(1 - iy, ic) + z * Z, Z, Z)
    ozy = put(xo.at[r0, :], xo.at[r0, :], ZN)
    oyc.wait_recv()
    r1 = ds(quarter(1 - iy, 1 - ic) + z * Z, Z, Z)
    ozc = put(xo.at[r1, :], xo.at[r1, :], ZN)
    for u in range(5, 10):
        got_x(u)
        got_y(u)
        got_d(u - 5)
    for u in range(5, 10):
        got_d(u)
    for c in (oc, ozy, ozc):
        c.wait_recv()
    for c in qcr:
        c.wait_recv()
    settle(list(sends))


def solution(mesh):
    def body(x, g1, g2, w_gate, w_up, w_down, o, w_o, w_qkv):
        spread = lambda v: lax.broadcast_in_dim(v, (8, B), (1,))
        g = jnp.where(lax.broadcasted_iota(jnp.int32, (8, B), 0) == 0, spread(g1), spread(g2))
        hbm, vmem = pl.BlockSpec(memory_space=pltpu.HBM), pl.BlockSpec(memory_space=pltpu.VMEM)
        keep = lambda v: pltpu.with_memory_space_constraint(v, pltpu.HBM)
        outs = pl.pallas_call(
            _kernel,
            out_shape=(pltpu.VMEM((T, B), BF), pltpu.VMEM((T, Q // 2), BF), pltpu.HBM((3, K2, B), BF),
                       pltpu.HBM((8, B, QC), BF), pltpu.HBM((2, D, 2 * PC), BF)),
            in_specs=[hbm, vmem] + [hbm] * 6,
            out_specs=(vmem, vmem, hbm, hbm, hbm),
            scratch_shapes=[
                pltpu.VMEM((R, D), BF), pltpu.VMEM((R, D), BF), pltpu.VMEM((2 * D, 2 * PC), BF),
                pltpu.VMEM((R, FP), BF), pltpu.VMEM((Z, 12 * S), F32), pltpu.VMEM((Z, 12 * S), F32),
                pltpu.VMEM((Z, 4 * S), F32), pltpu.VMEM((8, D), F32),
                pltpu.SemaphoreType.DMA((NREMOTE,)), pltpu.SemaphoreType.DMA((NREMOTE,)),
                pltpu.SemaphoreType.DMA((NLOCAL,)),
            ],
            compiler_params=pltpu.CompilerParams(collective_id=0, has_side_effects=True,
                                                 vmem_limit_bytes=VMEM_LIMIT),
        )(keep(x), g, *[keep(v) for v in (w_gate, w_up, w_down, o, w_o, w_qkv)])
        return outs[0], outs[1]

    in_specs = (P(None, 'h'), P('h'), P('h'), P('h', 'f'), P('h', 'f'), P('f', 'h'),
                P(None, 'f'), P('f', 'h'), P('h', 'f'))
    return jax.shard_map(body, mesh=mesh, in_specs=in_specs,
                         out_specs=(P(None, 'h'), P(None, 'f')), check_vma=False)
```

```python
import jax
import jax.numpy as jnp
from jax import lax
from jax.experimental import pallas as pl
from jax.experimental.pallas import tpu as pltpu
from jax.sharding import PartitionSpec as P

EPS = 1e-6
BF, F32 = jnp.bfloat16, jnp.float32
MESH = pl.DeviceIdType.MESH
NREMOTE, NLOCAL = 288, 128

T, D, FF, HD, Q = 4096, 3072, 8192, 3072, 5120
B = D // 8
R = T // 4
Z = R // 2
FP = FF // 2
PIECES = 4
PC = FP // 2 // PIECES
K2 = FP + HD // 2
S = 128
QC = Q // 4
M = 256
FX, OC, S2 = FP // 2, HD // 2, 2 * S
QT = 256
QN = QC // QT
EARLY, LATE = (0, 1, 4, 5), (2, 3, 6, 7)
QSLOT = ((0, 512), (D, 512), (0, 768), (D, 768), (0, 0))
VMEM_LIMIT = 67043328 - T * (B + Q // 2) * 2 - 65536
UNITS = ((0, 0, M, 0), (0, M, M, 0)) + tuple((0, 0, Z, t) for t in range(1, 5)) + (
    tuple((1, 0, Z, t) for t in range(4)) + ((1, 0, M, 4), (1, M, M, 4)))
XFIRST = (3, 7)


def _dot(a, b):
    return jnp.dot(a, b, preferred_element_type=F32)


def _kernel(x, g, wg, wu, wd, o, wo, wq, xo, qo, dl, ql, wh,
            A, N, W, act, ys, yr, yo, gv, send, recv, loc):
    h = lax.axis_index('h')
    z = lax.axis_index('f')
    iy, ix, ic = lax.div(h, 4), lax.rem(lax.div(h, 2), 2), lax.rem(h, 2)

    def dev(kx, ky, kc):
        py = 1 - iy if ky else iy
        px = 1 - ix if kx else ix
        pc = 1 - ic if kc else ic
        return {'h': py * 4 + px * 2 + pc}

    XN, YN, CN, YCN, ZN = dev(1, 0, 0), dev(0, 1, 0), dev(0, 0, 1), dev(0, 1, 1), {'f': 1 - z}
    count = [0, 0]
    sends = []

    def put(src, dst, to):
        i = count[0]
        count[0] += 1
        c = pltpu.make_async_remote_copy(src, dst, send.at[i], recv.at[i], device_id=to, device_id_type=MESH)
        c.start()
        sends.append(c)
        return c

    def load(src, dst):
        i = count[1]
        count[1] += 1
        c = pltpu.make_async_copy(src, dst, loc.at[i])
        c.start()
        return c

    def settle(cs):
        for c in cs:
            c.wait_send()
            sends[:] = [d for d in sends if d is not c]

    def al(v, m):
        return pl.multiple_of(v, m)

    def ds(start, size, m):
        return pl.ds(al(start, m), size)

    def quarter(py, pc):
        return pc * (2 * R) + py * R

    mine = quarter(iy, ic)
    zr = ds(z * Z, Z, Z)
    zo = ds((1 - z) * Z, Z, Z)

    bar = pltpu.get_barrier_semaphore()
    for k in range(1, 8):
        pl.semaphore_signal(bar, inc=1, device_id=dev(k & 1, (k >> 1) & 1, k >> 2), device_id_type=MESH)
    pl.semaphore_signal(bar, inc=1, device_id=ZN, device_id_type=MESH)
    pl.semaphore_wait(bar, 8)

    def col(p):
        return pl.ds(p * B, B)

    x4 = put(x.at[ds(quarter(iy, 1 - ic), R, R), :], A.at[:, col(4)], CN)
    x2 = put(x.at[ds(quarter(1 - iy, ic) + z * Z, Z, Z), :], A.at[zr, col(2)], YN)
    x6 = put(x.at[ds(quarter(1 - iy, 1 - ic) + z * Z, Z, Z), :], A.at[zr, col(6)], YCN)
    x1 = put(x.at[ds(mine + z * Z, Z, Z), :], A.at[zr, col(1)], XN)
    x0 = load(x.at[ds(mine, R, R), :], A.at[:, col(0)])

    def wrow(j, a, n):
        return pl.ds((j % 2) * D + a, n)

    def wref(j, a, n, c=slice(None)):
        return W.at[wrow(j, a, n), c] if j < 2 else wh.at[j - 2, pl.ds(a, n), c]

    wl, wx, wyo, wyf, wc = {}, {}, {}, {}, {}
    GC, UC = pl.ds(0, PC), pl.ds(PC, PC)

    def wcol(j, other):
        return ds(((1 - ix) if other else ix) * FX + j * PC, PC, PC)

    def w_load(j):
        c0 = wcol(j, 0)
        wl[j] = [load(wg.at[:, c0], W.at[wrow(j, 0, B), GC]), load(wu.at[:, c0], W.at[wrow(j, 0, B), UC])]

    def w_x(j):
        c1 = wcol(j, 1)
        wx[j] = [put(wg.at[:, c1], wref(j, B, B, GC), XN), put(wu.at[:, c1], wref(j, B, B, UC), XN)]

    def w_yown(j):
        if j < 2:
            for c in wl[j]:
                c.wait()
            wyo[j] = [put(wref(j, 0, B), wref(j, 2 * B, B), YN)]
            wc[j] = [put(wref(j, 0, B), wref(j, 4 * B, B), CN)]
        else:
            c0 = wcol(j, 0)
            wyo[j] = [put(wg.at[:, c0], wref(j, 2 * B, B, GC), YN), put(wu.at[:, c0], wref(j, 2 * B, B, UC), YN)]
            wc[j] = [put(wg.at[:, c0], wref(j, 4 * B, B, GC), CN), put(wu.at[:, c0], wref(j, 4 * B, B, UC), CN)]

    def w_xgot(j):
        for c in wx[j]:
            c.wait_recv()
        wyf[j] = [put(wref(j, B, B), wref(j, 3 * B, B), YN)]
        wc[j].append(put(wref(j, B, B), wref(j, 5 * B, B), CN))

    def w_block(j, k, n=1):
        return load(wref(j, k * B, n * B), W.at[wrow(j, k * B, n * B), :])

    def w_ygot(j):
        for c in wyo[j]:
            c.wait_recv()
        own = len(wc[j])
        wc[j].append(put(wref(j, 2 * B, B), wref(j, 6 * B, B), CN))
        loads = []
        if j >= 2:
            w_load(j)
            for c in wc[j][:own]:
                c.wait_recv()
            loads = wl[j] + [w_block(j, 1, 2), w_block(j, 4, 2)]
        for c in wyf[j]:
            c.wait_recv()
        wc[j].append(put(wref(j, 3 * B, B), wref(j, 7 * B, B), CN))
        if j >= 2:
            loads.append(w_block(j, 3))
        for c in wc[j] if j < 2 else wc[j][own:]:
            c.wait_recv()
        if j >= 2:
            loads.append(w_block(j, 6, 2))
        for c in loads:
            c.wait()

    w_load(0)
    w_load(1)
    w_x(0)
    gs = [put(g, gv.at[:, col(k)], dev(k & 1, (k >> 1) & 1, k >> 2)) for k in range(1, 8)]
    g0 = load(g, gv.at[:, col(0)])
    w_yown(0)
    w_yown(1)

    dc = [put(wd, dl.at[1, pl.ds(0, FP), :], CN), put(wo, dl.at[1, pl.ds(FP, OC), :], CN)]
    qc0 = put(wq.at[:, ds(ix * QC, QC, QC)], ql.at[4], CN)

    x4.wait_recv()
    x5 = put(A.at[zr, col(4)], A.at[zr, col(5)], XN)
    zs = []

    def zput(p):
        zs.append(put(A.at[zr, col(p)], A.at[zr, col(p)], ZN))

    x1.wait_recv()
    zput(1)
    x2.wait_recv()
    x3 = put(A.at[zr, col(2)], A.at[zr, col(3)], XN)
    zput(2)
    x6.wait_recv()
    x7 = put(A.at[zr, col(6)], A.at[zr, col(7)], XN)
    zput(6)
    for j in range(1, PIECES):
        w_x(j)
    w_xgot(0)
    w_yown(2)
    x5.wait_recv()
    zput(5)
    x3.wait_recv()
    zput(3)
    x7.wait_recv()
    zput(7)
    for c in gs:
        c.wait_recv()
    g0.wait()
    x0.wait()
    for c in zs:
        c.wait_recv()

    def norm(row, n, gi):
        gain = gv[gi:gi + 1, :]

        def body(i, _):
            rows = ds(row + i * 32, 32, 32)
            v = A[rows, :].astype(F32)
            ss = jnp.sum(v * v, axis=-1, keepdims=True)
            N[rows, :] = (v * lax.rsqrt(ss / D + EPS) * gain).astype(BF)
            return 0

        lax.fori_loop(0, n // 32, body, 0)

    norm(0, R, 0)

    def gate_up(j, half):
        def body(t, _):
            rows = ds(half * Z + lax.div(t, 2) * M, M, M)
            c = lax.rem(t, 2) * M
            n = N[rows, :]
            gt = _dot(n, W[wrow(j, 0, D), ds(c, M, M)])
            up = _dot(n, W[wrow(j, 0, D), ds(PC + c, M, M)])
            act[rows, ds(j * PC + c, M, M)] = (jax.nn.silu(gt) * up).astype(BF)
            return 0

        lax.fori_loop(0, (Z // M) * (PC // M), body, 0)

    dy, dyc, dloads = {}, {}, {}

    def down_y(p):
        c = pl.ds(p * S, S)
        dy[p] = [put(wd.at[:, c], dl.at[0, pl.ds(0, FP), c], YN),
                 put(wo.at[:, c], dl.at[0, pl.ds(FP, OC), c], YN)]

    def dslot(ky, p):
        return ((ky * 3 + p) % 4) * S2

    def down_load(ky, p):
        out = []
        for kc in range(2):
            c = pl.ds(p * S, S)
            if ky == 0 and kc == 0:
                top, bot = wd, wo.at[:, c]
            else:
                k = ky + 2 * kc - 1
                top, bot = dl.at[k], dl.at[k, pl.ds(FP, OC), c]
            to = pl.ds(dslot(ky, p) + kc * S, S)
            out.append(load(top.at[ds(ix * FX, FX, FX), c], W.at[pl.ds(0, FX), to]))
            out.append(load(top.at[ds((1 - ix) * FX, FX, FX), c], W.at[pl.ds(FX, FX), to]))
            out.append(load(bot, W.at[pl.ds(FP, OC), to]))
        dloads[ky, p] = out

    def w_settle(j):
        settle(wx[j] + wyo[j] + wyf[j] + wc[j])

    acts = {}

    def act_put(j, half):
        rows = zo if half else zr
        acts[j, half] = put(act.at[rows, pl.ds(j * PC, PC)], act.at[rows, pl.ds(FX + j * PC, PC)], XN)

    for j in range(PIECES):
        if j + 1 < PIECES:
            w_xgot(j + 1)
        if j == 0:
            w_yown(3)
        if j == 2:
            w_settle(0)
            for p in range(3):
                down_y(p)
        if j == 3:
            w_settle(1)
        w_ygot(j)
        gate_up(j, 1 - z)
        if j == 0:
            settle(zs + [x1, x2, x3, x4, x5, x6, x7] + gs)
        act_put(j, 1)
        if j == 3:
            act_put(2, 0)
        gate_up(j, z)
        if j != 2:
            act_put(j, 0)

    qx = put(wq.at[:, ds((1 - ix) * QC, QC, QC)], ql.at[1], XN)
    for c in dc:
        c.wait_recv()
    for p in range(3):
        down_load(0, p)
    ol = load(o.at[ds(mine, R, R), :], N.at[:, pl.ds(0, OC)])

    rs = {}

    def step(ky, p):
        return (ky * 3 + p) * S2

    def down(ky, p, half, dst, at, i0=0, n=Z // M):
        def f(i, _):
            c = pl.ds(dslot(ky, p), S2)
            rows = ds(half * Z + i * M, M, M)
            dst[ds(i * M, M, M), pl.ds(at, S2)] = (
                _dot(act[rows, :], W[pl.ds(0, FP), c]) + _dot(N[rows, pl.ds(0, OC)], W[pl.ds(FP, OC), c]))
            return 0
        lax.fori_loop(i0, i0 + n, f, 0)

    def parts(ky, p):
        return ((0, M), (M, M)) if (ky, p) == (1, 2) else ((0, Z),)

    def down_far(ky, p):
        for c in dloads[ky, p]:
            c.wait()
        s = pl.ds(step(ky, p), S2)
        for r, n in parts(ky, p):
            down(ky, p, 1 - z, ys, step(ky, p), r // M, n // M)
            rs[ky, p, r] = put(ys.at[pl.ds(r, n), s], yr.at[pl.ds(r, n), s], ZN)

    def near(ky, p):
        return ((ky * 3 + p) % 2) * S2

    def down_near(ky, p):
        down(ky, p, z, yo, near(ky, p))

    def acol(ky, p, kc, kx=0):
        return pl.ds((2 * ky + 4 * kc + kx) * B + p * S, S)

    xx, xz, xf = {}, {}, {}

    def finish_part(ky, p, r0, n):
        rs[ky, p, r0].wait_recv()

        def f(i, _):
            r = ds(r0 + i * 64, 64, 64)
            ra = ds(z * Z + r0 + i * 64, 64, 64)
            for kc in range(2):
                c = acol(ky, p, kc)
                mine_y = yo[r, pl.ds(near(ky, p) + kc * S, S)]
                A[ra, c] = (A[ra, c].astype(F32) + (mine_y + yr[r, pl.ds(step(ky, p) + kc * S, S)])).astype(BF)
            return 0

        lax.fori_loop(0, n // 64, f, 0)
        rows = ds(z * Z + r0, n, n)
        for kc in range(2):
            xx[ky, p, kc, r0] = put(A.at[rows, acol(ky, p, kc)], A.at[rows, acol(ky, p, kc, 1)], XN)

    def finish(ky, p):
        for r0, n in parts(ky, p):
            finish_part(ky, p, r0, n)

    def z_own(ky, p):
        for kc in range(2):
            c = acol(ky, p, kc)
            xz[ky, p, kc] = put(A.at[zr, c], A.at[zr, c], ZN)

    def x_got_part(ky, p, r0):
        for kc in range(2):
            xx[ky, p, kc, r0].wait_recv()

    def x_got(ky, p):
        for r0, _ in parts(ky, p):
            x_got_part(ky, p, r0)

    def z_far(ky, p):
        for kc in range(2):
            c = acol(ky, p, kc, 1)
            xf[ky, p, kc] = put(A.at[zr, c], A.at[zr, c], ZN)

    def down_ygot(p):
        for c in dy[p]:
            c.wait_recv()
        c = pl.ds(p * S, S)
        dyc[p] = put(dl.at[0, :, c], dl.at[2, :, c], CN)

    def down_ready(p):
        dyc[p].wait_recv()
        down_load(1, p)

    ol.wait()
    for j in range(PIECES):
        acts[j, 1].wait_recv()
    for p in range(3):
        down_far(0, p)
    down_ygot(0)
    down_ready(0)
    down_far(1, 0)
    for j in range(PIECES):
        acts[j, 0].wait_recv()
    down_near(0, 0)
    down_near(0, 1)
    finish(0, 0)
    down_near(0, 2)
    finish(0, 1)
    down_near(1, 0)
    finish(0, 2)
    z_own(0, 0)
    z_own(0, 1)

    qyo, qyf, qcy, qloads = {}, {}, {}, {}

    def tile(t):
        return pl.ds(t * QT, QT)

    def qw_y(gi):
        qyo[gi] = put(wq.at[:, ds(ix * QC + gi * QT, QT, QT)], ql.at[2, :, tile(gi)], YN)
        qyf[gi] = put(ql.at[1, :, tile(gi)], ql.at[3, :, tile(gi)], YN)

    def qw_ygot(gi):
        qyo[gi].wait_recv()
        a1 = put(ql.at[2, :, tile(gi)], ql.at[6, :, tile(gi)], CN)
        qyf[gi].wait_recv()
        a2 = put(ql.at[3, :, tile(gi)], ql.at[7, :, tile(gi)], CN)
        qcy[gi] = (a1, a2)

    def slot(t, k):
        r, c = QSLOT[t]
        return W.at[pl.ds(r + k * B, B), pl.ds(c, QT)]

    def qload(t, ks):
        for k in ks:
            src = ql.at[k, :, tile(t)] if k else wq.at[:, ds(ix * QC + t * QT, QT, QT)]
            qloads.setdefault(t, []).append(load(src, slot(t, k)))

    qx.wait_recv()
    qc1 = put(ql.at[1], ql.at[5], CN)
    for gi in range(QN):
        qw_y(gi)
    qc0.wait_recv()
    qc1.wait_recv()
    for gi in range(4):
        qload(gi, EARLY)

    down_ygot(1)
    down_ready(1)
    down_far(1, 1)
    z_own(0, 2)
    x_got(0, 0)
    z_far(0, 0)
    finish(1, 0)
    down_near(1, 1)
    qload(4, EARLY)
    x_got(0, 1)
    x_got(0, 2)
    finish(1, 1)
    down_ygot(2)
    down_ready(2)
    down_far(1, 2)
    z_far(0, 1)
    z_far(0, 2)
    for p in range(2):
        z_own(1, p)
    for p in range(2):
        x_got(1, p)
        z_far(1, p)
    down_near(1, 2)
    def qw_ready(gi):
        for c in qcy[gi]:
            c.wait_recv()
        qload(gi, LATE)

    qw_ygot(0)
    qw_ready(0)

    qxr, qyr, qdr, qcr = {}, {}, {}, []

    def at(u, fy, fx):
        far, r, n, t = UNITS[u]
        half = 1 - z if far else z
        py = 1 - iy if fy else iy
        px = 1 - ix if fx else ix
        return qo.at[ds(quarter(py, ic) + half * Z + r, n, n), ds(px * QC + t * QT, QT, QT)]

    def unit(u):
        far, r0, n, t = UNITS[u]
        for c in qloads.pop(t, ()):
            c.wait()
        base = (1 - z if far else z) * Z + r0

        def f(i, _):
            r, c = QSLOT[t]
            w = W[pl.ds(r, D), pl.ds(c, QT)]
            to = qo.at[ds(mine + base + i * M, M, M), ds(ix * QC + t * QT, QT, QT)]
            to[...] = _dot(N[ds(base + i * M, M, M), :], w).astype(BF)
            return 0

        lax.fori_loop(0, n // M, f, 0)
        ref = at(u, 0, 0)
        qxr[u] = put(ref, ref, XN)
        qyr[u] = put(ref, ref, YN)
        qcr.append(put(ref, ref, CN))

    def got_x(*us):
        for u in us:
            qxr[u].wait_recv()
            ref = at(u, 0, 1)
            if u in XFIRST:
                qdr[u] = put(ref, ref, YN)
            qcr.append(put(ref, ref, CN))

    def got_y(*us):
        for u in us:
            qyr[u].wait_recv()
            ref = at(u, 1, 0)
            if u not in XFIRST:
                qdr[u] = put(ref, ref, XN)
            qcr.append(put(ref, ref, CN))

    def got_d(*us):
        for u in us:
            qdr[u].wait_recv()
            ref = at(u, 1, 1)
            qcr.append(put(ref, ref, CN))

    finish(1, 2)
    z_own(1, 2)
    x_got_part(1, 2, 0)
    qw_ygot(1)
    norm(z * Z, M, 1)
    unit(0)
    qw_ready(1)
    x_got_part(1, 2, M)
    z_far(1, 2)
    norm(z * Z + M, M, 1)
    unit(1)
    unit(2)
    qw_ygot(2)
    qw_ready(2)
    got_x(0, 1)
    unit(3)
    qw_ygot(3)
    qw_ready(3)
    unit(4)
    got_x(2)
    qw_ygot(4)
    qw_ready(4)
    unit(5)
    orow = ds(mine + z * Z, Z, Z)
    oy = put(A.at[zr, col(2)], xo.at[orow, :], YN)
    oyc = put(A.at[zr, col(6)], xo.at[orow, :], YCN)
    got_x(3)
    got_y(0, 1)
    got_x(4)
    got_y(2, 3)
    got_x(5)
    got_y(4)
    for k in xz:
        xz[k].wait_recv()
    got_y(5)
    for k in xf:
        xf[k].wait_recv()
    norm((1 - z) * Z, Z, 1)
    unit(6)
    unit(7)
    unit(8)
    got_d(0, 1, 2)
    unit(9)
    unit(10)
    unit(11)
    oc = put(A.at[:, col(4)], xo.at[ds(mine, R, R), :], CN)

    def keep(i, _):
        xo[ds(mine + i * M, M, M), :] = A[ds(i * M, M, M), col(0)]
        return 0

    lax.fori_loop(0, R // M, keep, 0)
    got_x(6)
    oy.wait_recv()
    r0 = ds(quarter(1 - iy, ic) + z * Z, Z, Z)
    ozy = put(xo.at[r0, :], xo.at[r0, :], ZN)
    oyc.wait_recv()
    r1 = ds(quarter(1 - iy, 1 - ic) + z * Z, Z, Z)
    ozc = put(xo.at[r1, :], xo.at[r1, :], ZN)
    got_d(3, 4, 5)
    got_x(7)
    got_y(6)
    got_x(8)
    got_y(7)
    got_x(9)
    got_y(8)
    got_x(10, 11)
    got_y(9, 10, 11)
    got_d(*range(6, 12))
    for c in (oc, ozy, ozc):
        c.wait_recv()
    for c in qcr:
        c.wait_recv()
    settle(list(sends))


def solution(mesh):
    def body(x, g1, g2, w_gate, w_up, w_down, o, w_o, w_qkv):
        spread = lambda v: lax.broadcast_in_dim(v, (8, B), (1,))
        g = jnp.where(lax.broadcasted_iota(jnp.int32, (8, B), 0) == 0, spread(g1), spread(g2))
        hbm, vmem = pl.BlockSpec(memory_space=pltpu.HBM), pl.BlockSpec(memory_space=pltpu.VMEM)
        keep = lambda v: pltpu.with_memory_space_constraint(v, pltpu.HBM)
        outs = pl.pallas_call(
            _kernel,
            out_shape=(pltpu.VMEM((T, B), BF), pltpu.VMEM((T, Q // 2), BF), pltpu.HBM((3, K2, B), BF),
                       pltpu.HBM((8, B, QC), BF), pltpu.HBM((2, D, 2 * PC), BF)),
            in_specs=[hbm, vmem] + [hbm] * 6,
            out_specs=(vmem, vmem, hbm, hbm, hbm),
            scratch_shapes=[
                pltpu.VMEM((R, D), BF), pltpu.VMEM((R, D), BF), pltpu.VMEM((2 * D, 2 * PC), BF),
                pltpu.VMEM((R, FP), BF), pltpu.VMEM((Z, 6 * S2), F32), pltpu.VMEM((Z, 6 * S2), F32),
                pltpu.VMEM((Z, 4 * S), F32), pltpu.VMEM((8, D), F32),
                pltpu.SemaphoreType.DMA((NREMOTE,)), pltpu.SemaphoreType.DMA((NREMOTE,)),
                pltpu.SemaphoreType.DMA((NLOCAL,)),
            ],
            compiler_params=pltpu.CompilerParams(collective_id=0, has_side_effects=True,
                                                 vmem_limit_bytes=VMEM_LIMIT),
        )(keep(x), g, *[keep(v) for v in (w_gate, w_up, w_down, o, w_o, w_qkv)])
        return outs[0], outs[1]

    in_specs = (P(None, 'h'), P('h'), P('h'), P('h', 'f'), P('h', 'f'), P('f', 'h'),
                P(None, 'f'), P('f', 'h'), P('h', 'f'))
    return jax.shard_map(body, mesh=mesh, in_specs=in_specs,
                         out_specs=(P(None, 'h'), P(None, 'f')), check_vma=False)
```

```python
import jax
import jax.numpy as jnp
from jax import lax
from jax.experimental import pallas as pl
from jax.experimental.pallas import tpu as pltpu
from jax.sharding import PartitionSpec as P

EPS = 1e-6
BF, F32 = jnp.bfloat16, jnp.float32
MESH = pl.DeviceIdType.MESH
NREMOTE, NLOCAL, NWRITE = 288, 128, 8

T, D, FF, HD, Q = 4096, 3072, 8192, 3072, 5120
B = D // 8
R = T // 4
Z = R // 2
FP = FF // 2
PIECES = 4
PC = FP // 2 // PIECES
K2 = FP + HD // 2
S = 128
QC = Q // 4
M = 256
FX, OC, S2 = FP // 2, HD // 2, 2 * S
QT = 256
QN = QC // QT
EARLY, LATE = (0, 1, 4, 5), (2, 3, 6, 7)
QSLOT = ((0, 512), (D, 512), (0, 768), (D, 768), (0, 0))
VMEM_LIMIT = 67043328 - T * (B + Q // 2) * 2 - 65536
UNITS = ((0, 0, M, 0), (0, M, M, 0)) + tuple((0, 0, Z, t) for t in range(1, 5)) + (
    tuple((1, 0, Z, t) for t in range(4)) + ((1, 0, M, 4), (1, M, M, 4)))
XFIRST = (3, 7)


def _dot(a, b):
    return jnp.dot(a, b, preferred_element_type=F32)


def _kernel(x, ga, gb, wg, wu, wd, o, wo, wq, xo, qo, dl, ql, wh,
            A, N, W, act, ys, yr, yo, gv, send, recv, loc):
    h = lax.axis_index('h')
    z = lax.axis_index('f')
    iy, ix, ic = lax.div(h, 4), lax.rem(lax.div(h, 2), 2), lax.rem(h, 2)

    def dev(kx, ky, kc):
        py = 1 - iy if ky else iy
        px = 1 - ix if kx else ix
        pc = 1 - ic if kc else ic
        return {'h': py * 4 + px * 2 + pc}

    XN, YN, CN, YCN, ZN = dev(1, 0, 0), dev(0, 1, 0), dev(0, 0, 1), dev(0, 1, 1), {'f': 1 - z}
    count = [0, 0]
    sends = []

    def put(src, dst, to):
        i = count[0]
        count[0] += 1
        c = pltpu.make_async_remote_copy(src, dst, send.at[i], recv.at[i], device_id=to, device_id_type=MESH)
        c.start()
        sends.append(c)
        return c

    def load(src, dst):
        i = count[1]
        count[1] += 1
        c = pltpu.make_async_copy(src, dst, loc.at[i])
        c.start()
        return c

    def settle(cs):
        for c in cs:
            c.wait_send()
            sends[:] = [d for d in sends if d is not c]

    def al(v, m):
        return pl.multiple_of(v, m)

    def ds(start, size, m):
        return pl.ds(al(start, m), size)

    def quarter(py, pc):
        return pc * (2 * R) + py * R

    mine = quarter(iy, ic)
    zr = ds(z * Z, Z, Z)
    zo = ds((1 - z) * Z, Z, Z)

    bar = pltpu.get_barrier_semaphore()
    for k in range(1, 8):
        pl.semaphore_signal(bar, inc=1, device_id=dev(k & 1, (k >> 1) & 1, k >> 2), device_id_type=MESH)
    pl.semaphore_signal(bar, inc=1, device_id=ZN, device_id_type=MESH)
    pl.semaphore_wait(bar, 8)

    def col(p):
        return pl.ds(p * B, B)

    x4 = put(x.at[ds(quarter(iy, 1 - ic), R, R), :], A.at[:, col(4)], CN)
    x2 = put(x.at[ds(quarter(1 - iy, ic) + z * Z, Z, Z), :], A.at[zr, col(2)], YN)
    x6 = put(x.at[ds(quarter(1 - iy, 1 - ic) + z * Z, Z, Z), :], A.at[zr, col(6)], YCN)
    x1 = put(x.at[ds(mine + z * Z, Z, Z), :], A.at[zr, col(1)], XN)
    x0 = load(x.at[ds(mine, R, R), :], A.at[:, col(0)])

    def wrow(j, a, n):
        return pl.ds((j % 2) * D + a, n)

    def wref(j, a, n, c=slice(None)):
        return W.at[wrow(j, a, n), c] if j < 2 else wh.at[j - 2, pl.ds(a, n), c]

    wl, wx, wyo, wyf, wc = {}, {}, {}, {}, {}
    GC, UC = pl.ds(0, PC), pl.ds(PC, PC)

    def wcol(j, other):
        return ds(((1 - ix) if other else ix) * FX + j * PC, PC, PC)

    def w_load(j):
        c0 = wcol(j, 0)
        wl[j] = [load(wg.at[:, c0], W.at[wrow(j, 0, B), GC]), load(wu.at[:, c0], W.at[wrow(j, 0, B), UC])]

    def w_x(j):
        c1 = wcol(j, 1)
        wx[j] = [put(wg.at[:, c1], wref(j, B, B, GC), XN), put(wu.at[:, c1], wref(j, B, B, UC), XN)]

    def w_yown(j):
        if j < 2:
            for c in wl[j]:
                c.wait()
            wyo[j] = [put(wref(j, 0, B), wref(j, 2 * B, B), YN)]
            wc[j] = [put(wref(j, 0, B), wref(j, 4 * B, B), CN)]
        else:
            c0 = wcol(j, 0)
            wyo[j] = [put(wg.at[:, c0], wref(j, 2 * B, B, GC), YN), put(wu.at[:, c0], wref(j, 2 * B, B, UC), YN)]
            wc[j] = [put(wg.at[:, c0], wref(j, 4 * B, B, GC), CN), put(wu.at[:, c0], wref(j, 4 * B, B, UC), CN)]

    def w_xgot(j):
        for c in wx[j]:
            c.wait_recv()
        wyf[j] = [put(wref(j, B, B), wref(j, 3 * B, B), YN)]
        wc[j].append(put(wref(j, B, B), wref(j, 5 * B, B), CN))

    def w_block(j, k, n=1):
        return load(wref(j, k * B, n * B), W.at[wrow(j, k * B, n * B), :])

    def w_ygot(j):
        for c in wyo[j]:
            c.wait_recv()
        own = len(wc[j])
        wc[j].append(put(wref(j, 2 * B, B), wref(j, 6 * B, B), CN))
        loads = []
        if j >= 2:
            w_load(j)
            for c in wc[j][:own]:
                c.wait_recv()
            loads = wl[j] + [w_block(j, 1, 2), w_block(j, 4, 2)]
        for c in wyf[j]:
            c.wait_recv()
        wc[j].append(put(wref(j, 3 * B, B), wref(j, 7 * B, B), CN))
        if j >= 2:
            loads.append(w_block(j, 3))
        for c in wc[j] if j < 2 else wc[j][own:]:
            c.wait_recv()
        if j >= 2:
            loads.append(w_block(j, 6, 2))
        for c in loads:
            c.wait()

    w_load(0)
    w_load(1)
    w_x(0)
    gs = [put(v, gv.at[i, k], dev(k & 1, (k >> 1) & 1, k >> 2)) for k in range(1, 8) for i, v in enumerate((ga, gb))]
    gv[0, 0] = ga[...]
    gv[1, 0] = gb[...]
    w_yown(0)
    w_yown(1)

    dc = [put(wd, dl.at[1, pl.ds(0, FP), :], CN), put(wo, dl.at[1, pl.ds(FP, OC), :], CN)]
    qc0 = put(wq.at[:, ds(ix * QC, QC, QC)], ql.at[4], CN)

    x4.wait_recv()
    x5 = put(A.at[zr, col(4)], A.at[zr, col(5)], XN)
    zs = []

    def zput(p):
        zs.append(put(A.at[zr, col(p)], A.at[zr, col(p)], ZN))

    x1.wait_recv()
    zput(1)
    x2.wait_recv()
    x3 = put(A.at[zr, col(2)], A.at[zr, col(3)], XN)
    zput(2)
    x6.wait_recv()
    x7 = put(A.at[zr, col(6)], A.at[zr, col(7)], XN)
    zput(6)
    for j in range(1, PIECES):
        w_x(j)
    w_xgot(0)
    w_yown(2)
    x5.wait_recv()
    zput(5)
    x3.wait_recv()
    zput(3)
    x7.wait_recv()
    zput(7)
    for c in gs:
        c.wait_recv()
    x0.wait()
    for c in zs:
        c.wait_recv()

    def norm(row, n, gi):
        gain = jnp.concatenate([gv[gi, k, i:i + 1, :] for k in range(8) for i in range(3)], 1)

        def body(i, _):
            rows = ds(row + i * 32, 32, 32)
            v = A[rows, :].astype(F32)
            ss = jnp.sum(v * v, axis=-1, keepdims=True)
            N[rows, :] = (v * lax.rsqrt(ss / D + EPS) * gain).astype(BF)
            return 0

        lax.fori_loop(0, n // 32, body, 0)

    norm(0, R, 0)

    def gate_up(j, half):
        def body(t, _):
            rows = ds(half * Z + lax.div(t, 2) * M, M, M)
            c = lax.rem(t, 2) * M
            n = N[rows, :]
            gt = _dot(n, W[wrow(j, 0, D), ds(c, M, M)])
            up = _dot(n, W[wrow(j, 0, D), ds(PC + c, M, M)])
            act[rows, ds(j * PC + c, M, M)] = (jax.nn.silu(gt) * up).astype(BF)
            return 0

        lax.fori_loop(0, (Z // M) * (PC // M), body, 0)

    dy, dyc, dloads = {}, {}, {}

    def down_y(p):
        c = pl.ds(p * S, S)
        dy[p] = [put(wd.at[:, c], dl.at[0, pl.ds(0, FP), c], YN),
                 put(wo.at[:, c], dl.at[0, pl.ds(FP, OC), c], YN)]

    def dslot(ky, p):
        return ((ky * 3 + p) % 4) * S2

    def down_load(ky, p):
        out = []
        for kc in range(2):
            c = pl.ds(p * S, S)
            if ky == 0 and kc == 0:
                top, bot = wd, wo.at[:, c]
            else:
                k = ky + 2 * kc - 1
                top, bot = dl.at[k], dl.at[k, pl.ds(FP, OC), c]
            to = pl.ds(dslot(ky, p) + kc * S, S)
            out.append(load(top.at[ds(ix * FX, FX, FX), c], W.at[pl.ds(0, FX), to]))
            out.append(load(top.at[ds((1 - ix) * FX, FX, FX), c], W.at[pl.ds(FX, FX), to]))
            out.append(load(bot, W.at[pl.ds(FP, OC), to]))
        dloads[ky, p] = out

    def w_settle(j):
        settle(wx[j] + wyo[j] + wyf[j] + wc[j])

    acts = {}

    def act_put(j, half):
        rows = zo if half else zr
        acts[j, half] = put(act.at[rows, pl.ds(j * PC, PC)], act.at[rows, pl.ds(FX + j * PC, PC)], XN)

    for j in range(PIECES):
        if j + 1 < PIECES:
            w_xgot(j + 1)
        if j == 0:
            w_yown(3)
        if j == 2:
            w_settle(0)
            for p in range(3):
                down_y(p)
        if j == 3:
            w_settle(1)
        w_ygot(j)
        gate_up(j, 1 - z)
        if j == 0:
            settle(zs + [x1, x2, x3, x4, x5, x6, x7] + gs)
        act_put(j, 1)
        if j == 3:
            act_put(2, 0)
        gate_up(j, z)
        if j != 2:
            act_put(j, 0)

    qx = put(wq.at[:, ds((1 - ix) * QC, QC, QC)], ql.at[1], XN)
    for c in dc:
        c.wait_recv()
    for p in range(3):
        down_load(0, p)
    ol = load(o.at[ds(mine, R, R), :], N.at[:, pl.ds(0, OC)])

    rs = {}

    def step(ky, p):
        return (ky * 3 + p) * S2

    def down(ky, p, half, dst, at, i0=0, n=Z // M):
        def f(i, _):
            c = pl.ds(dslot(ky, p), S2)
            rows = ds(half * Z + i * M, M, M)
            dst[ds(i * M, M, M), pl.ds(at, S2)] = (
                _dot(act[rows, :], W[pl.ds(0, FP), c]) + _dot(N[rows, pl.ds(0, OC)], W[pl.ds(FP, OC), c]))
            return 0
        lax.fori_loop(i0, i0 + n, f, 0)

    def parts(ky, p):
        return ((0, M), (M, M)) if (ky, p) == (1, 2) else ((0, Z),)

    def down_far(ky, p):
        for c in dloads[ky, p]:
            c.wait()
        s = pl.ds(step(ky, p), S2)
        for r, n in parts(ky, p):
            down(ky, p, 1 - z, ys, step(ky, p), r // M, n // M)
            rs[ky, p, r] = put(ys.at[pl.ds(r, n), s], yr.at[pl.ds(r, n), s], ZN)

    def near(ky, p):
        return ((ky * 3 + p) % 2) * S2

    def down_near(ky, p):
        down(ky, p, z, yo, near(ky, p))

    def acol(ky, p, kc, kx=0):
        return pl.ds((2 * ky + 4 * kc + kx) * B + p * S, S)

    xx, xz, xf = {}, {}, {}

    def finish_part(ky, p, r0, n):
        rs[ky, p, r0].wait_recv()

        def f(i, _):
            r = ds(r0 + i * 64, 64, 64)
            ra = ds(z * Z + r0 + i * 64, 64, 64)
            for kc in range(2):
                c = acol(ky, p, kc)
                mine_y = yo[r, pl.ds(near(ky, p) + kc * S, S)]
                A[ra, c] = (A[ra, c].astype(F32) + (mine_y + yr[r, pl.ds(step(ky, p) + kc * S, S)])).astype(BF)
            return 0

        lax.fori_loop(0, n // 64, f, 0)
        rows = ds(z * Z + r0, n, n)
        for kc in range(2):
            xx[ky, p, kc, r0] = put(A.at[rows, acol(ky, p, kc)], A.at[rows, acol(ky, p, kc, 1)], XN)

    def finish(ky, p):
        for r0, n in parts(ky, p):
            finish_part(ky, p, r0, n)

    def z_own(ky, p):
        for kc in range(2):
            c = acol(ky, p, kc)
            xz[ky, p, kc] = put(A.at[zr, c], A.at[zr, c], ZN)

    def x_got_part(ky, p, r0):
        for kc in range(2):
            xx[ky, p, kc, r0].wait_recv()

    def x_got(ky, p):
        for r0, _ in parts(ky, p):
            x_got_part(ky, p, r0)

    def z_far(ky, p):
        for kc in range(2):
            c = acol(ky, p, kc, 1)
            xf[ky, p, kc] = put(A.at[zr, c], A.at[zr, c], ZN)

    def down_ygot(p):
        for c in dy[p]:
            c.wait_recv()
        c = pl.ds(p * S, S)
        dyc[p] = put(dl.at[0, :, c], dl.at[2, :, c], CN)

    def down_ready(p):
        dyc[p].wait_recv()
        down_load(1, p)

    ol.wait()
    for j in range(PIECES):
        acts[j, 1].wait_recv()
    for p in range(3):
        down_far(0, p)
    down_ygot(0)
    down_ready(0)
    down_far(1, 0)
    for j in range(PIECES):
        acts[j, 0].wait_recv()
    down_near(0, 0)
    down_near(0, 1)
    finish(0, 0)
    down_near(0, 2)
    finish(0, 1)
    down_near(1, 0)
    finish(0, 2)
    z_own(0, 0)
    z_own(0, 1)

    qyo, qyf, qcy, qloads = {}, {}, {}, {}

    def tile(t):
        return pl.ds(t * QT, QT)

    def qw_y(gi):
        qyo[gi] = put(wq.at[:, ds(ix * QC + gi * QT, QT, QT)], ql.at[2, :, tile(gi)], YN)
        qyf[gi] = put(ql.at[1, :, tile(gi)], ql.at[3, :, tile(gi)], YN)

    def qw_ygot(gi):
        qyo[gi].wait_recv()
        a1 = put(ql.at[2, :, tile(gi)], ql.at[6, :, tile(gi)], CN)
        qyf[gi].wait_recv()
        a2 = put(ql.at[3, :, tile(gi)], ql.at[7, :, tile(gi)], CN)
        qcy[gi] = (a1, a2)

    def slot(t, k):
        r, c = QSLOT[t]
        return W.at[pl.ds(r + k * B, B), pl.ds(c, QT)]

    def qload(t, ks):
        for k in ks:
            src = ql.at[k, :, tile(t)] if k else wq.at[:, ds(ix * QC + t * QT, QT, QT)]
            qloads.setdefault(t, []).append(load(src, slot(t, k)))

    qx.wait_recv()
    qc1 = put(ql.at[1], ql.at[5], CN)
    for gi in range(QN):
        qw_y(gi)
    qc0.wait_recv()
    qc1.wait_recv()
    for gi in range(4):
        qload(gi, EARLY)

    down_ygot(1)
    down_ready(1)
    down_far(1, 1)
    z_own(0, 2)
    x_got(0, 0)
    z_far(0, 0)
    finish(1, 0)
    down_near(1, 1)
    qload(4, EARLY)
    x_got(0, 1)
    x_got(0, 2)
    finish(1, 1)
    down_ygot(2)
    down_ready(2)
    down_far(1, 2)
    z_far(0, 1)
    z_far(0, 2)
    for p in range(2):
        z_own(1, p)
    for p in range(2):
        x_got(1, p)
        z_far(1, p)
    down_near(1, 2)
    def qw_ready(gi):
        for c in qcy[gi]:
            c.wait_recv()
        qload(gi, LATE)

    qw_ygot(0)
    qw_ready(0)

    qxr, qyr, qdr, qcr = {}, {}, {}, []

    def at(u, fy, fx):
        far, r, n, t = UNITS[u]
        half = 1 - z if far else z
        py = 1 - iy if fy else iy
        px = 1 - ix if fx else ix
        return qo.at[ds(quarter(py, ic) + half * Z + r, n, n), ds(px * QC + t * QT, QT, QT)]

    def unit(u):
        far, r0, n, t = UNITS[u]
        for c in qloads.pop(t, ()):
            c.wait()
        base = (1 - z if far else z) * Z + r0

        def f(i, _):
            r, c = QSLOT[t]
            w = W[pl.ds(r, D), pl.ds(c, QT)]
            to = qo.at[ds(mine + base + i * M, M, M), ds(ix * QC + t * QT, QT, QT)]
            to[...] = _dot(N[ds(base + i * M, M, M), :], w).astype(BF)
            return 0

        lax.fori_loop(0, n // M, f, 0)
        ref = at(u, 0, 0)
        qxr[u] = put(ref, ref, XN)
        qyr[u] = put(ref, ref, YN)
        qcr.append(put(ref, ref, CN))

    def got_x(*us):
        for u in us:
            qxr[u].wait_recv()
            ref = at(u, 0, 1)
            if u in XFIRST:
                qdr[u] = put(ref, ref, YN)
            qcr.append(put(ref, ref, CN))

    def got_y(*us):
        for u in us:
            qyr[u].wait_recv()
            ref = at(u, 1, 0)
            if u not in XFIRST:
                qdr[u] = put(ref, ref, XN)
            qcr.append(put(ref, ref, CN))

    def got_d(*us):
        for u in us:
            qdr[u].wait_recv()
            ref = at(u, 1, 1)
            qcr.append(put(ref, ref, CN))

    finish(1, 2)
    z_own(1, 2)
    x_got_part(1, 2, 0)
    qw_ygot(1)
    norm(z * Z, M, 1)
    unit(0)
    qw_ready(1)
    x_got_part(1, 2, M)
    z_far(1, 2)
    norm(z * Z + M, M, 1)
    unit(1)
    unit(2)
    qw_ygot(2)
    qw_ready(2)
    got_x(0, 1)
    unit(3)
    qw_ygot(3)
    qw_ready(3)
    unit(4)
    got_x(2)
    qw_ygot(4)
    qw_ready(4)
    unit(5)
    orow = ds(mine + z * Z, Z, Z)
    oy = put(A.at[zr, col(2)], xo.at[orow, :], YN)
    oyc = put(A.at[zr, col(6)], xo.at[orow, :], YCN)
    got_x(3)
    got_y(0, 1)
    got_x(4)
    got_y(2, 3)
    got_x(5)
    got_y(4)
    for k in xz:
        xz[k].wait_recv()
    got_y(5)
    for k in xf:
        xf[k].wait_recv()
    norm((1 - z) * Z, Z, 1)
    unit(6)
    unit(7)
    unit(8)
    got_d(0, 1, 2)
    unit(9)
    unit(10)
    unit(11)
    oc = put(A.at[:, col(4)], xo.at[ds(mine, R, R), :], CN)

    def keep(i, _):
        xo[ds(mine + i * M, M, M), :] = A[ds(i * M, M, M), col(0)]
        return 0

    lax.fori_loop(0, R // M, keep, 0)
    got_x(6)
    oy.wait_recv()
    r0 = ds(quarter(1 - iy, ic) + z * Z, Z, Z)
    ozy = put(xo.at[r0, :], xo.at[r0, :], ZN)
    oyc.wait_recv()
    r1 = ds(quarter(1 - iy, 1 - ic) + z * Z, Z, Z)
    ozc = put(xo.at[r1, :], xo.at[r1, :], ZN)
    got_d(3, 4, 5)
    got_x(7)
    got_y(6)
    got_x(8)
    got_y(7)
    got_x(9)
    got_y(8)
    got_x(10, 11)
    got_y(9, 10, 11)
    got_d(*range(6, 12))
    for c in (oc, ozy, ozc):
        c.wait_recv()
    for c in qcr:
        c.wait_recv()
    settle(list(sends))


def _write(a, b, ao, bo, sem):
    jobs = [(a, ao, pl.ds(0, T))] + [(b, bo, pl.ds(i * (T // NWRITE), T // NWRITE)) for i in range(NWRITE)]
    copies = [pltpu.make_async_copy(s.at[r, :], d.at[r, :], sem.at[i]) for i, (s, d, r) in enumerate(jobs)]
    for c in copies:
        c.start()
    for c in copies:
        c.wait()


def solution(mesh):
    def body(x, g1, g2, w_gate, w_up, w_down, o, w_o, w_qkv):
        hbm, vmem = pl.BlockSpec(memory_space=pltpu.HBM), pl.BlockSpec(memory_space=pltpu.VMEM)
        keep = lambda v: pltpu.with_memory_space_constraint(v, pltpu.HBM)
        outs = pl.pallas_call(
            _kernel,
            out_shape=(pltpu.VMEM((T, B), BF), pltpu.VMEM((T, Q // 2), BF), pltpu.HBM((3, K2, B), BF),
                       pltpu.HBM((8, B, QC), BF), pltpu.HBM((2, D, 2 * PC), BF)),
            in_specs=[hbm, vmem, vmem] + [hbm] * 6,
            out_specs=(vmem, vmem, hbm, hbm, hbm),
            scratch_shapes=[
                pltpu.VMEM((R, D), BF), pltpu.VMEM((R, D), BF), pltpu.VMEM((2 * D, 2 * PC), BF),
                pltpu.VMEM((R, FP), BF), pltpu.VMEM((Z, 6 * S2), F32), pltpu.VMEM((Z, 6 * S2), F32),
                pltpu.VMEM((Z, 4 * S), F32), pltpu.VMEM((2, 8, 3, 128), F32),
                pltpu.SemaphoreType.DMA((NREMOTE,)), pltpu.SemaphoreType.DMA((NREMOTE,)),
                pltpu.SemaphoreType.DMA((NLOCAL,)),
            ],
            compiler_params=pltpu.CompilerParams(collective_id=0, has_side_effects=True,
                                                 vmem_limit_bytes=VMEM_LIMIT),
        )(keep(x), g1.reshape(3, 128), g2.reshape(3, 128), *[keep(v) for v in (w_gate, w_up, w_down, o, w_o, w_qkv)])
        return pl.pallas_call(
            _write,
            out_shape=tuple(jax.ShapeDtypeStruct(v.shape, v.dtype) for v in outs[:2]),
            in_specs=[vmem, vmem],
            out_specs=(hbm, hbm),
            scratch_shapes=[pltpu.SemaphoreType.DMA((NWRITE + 1,))],
            compiler_params=pltpu.CompilerParams(vmem_limit_bytes=4 * T * D // 12),
        )(*[pltpu.with_memory_space_constraint(v, pltpu.VMEM) for v in outs[:2]])

    in_specs = (P(None, 'h'), P('h'), P('h'), P('h', 'f'), P('h', 'f'), P('f', 'h'),
                P(None, 'f'), P('f', 'h'), P('h', 'f'))
    return jax.shard_map(body, mesh=mesh, in_specs=in_specs,
                         out_specs=(P(None, 'h'), P(None, 'f')), check_vma=False)
```

```python
import jax
import jax.numpy as jnp
from jax import lax
from jax.experimental import pallas as pl
from jax.experimental.pallas import tpu as pltpu
from jax.sharding import PartitionSpec as P

EPS = 1e-6
BF, F32 = jnp.bfloat16, jnp.float32
MESH = pl.DeviceIdType.MESH
NREMOTE, NSEND, NLOCAL, NWRITE = 239, 96, 48, 8

T, D, FF, HD, Q = 4096, 3072, 8192, 3072, 5120
B = D // 8
R = T // 4
Z = R // 2
FP = FF // 2
PIECES = 4
PC = FP // 2 // PIECES
K2 = FP + HD // 2
S = 128
QC = Q // 4
M = 256
FX, OC, S2 = FP // 2, HD // 2, 2 * S
QT = 256
QN = QC // QT
EARLY, LATE = (0, 1, 4, 5), (2, 3, 6, 7)
QSLOT = ((0, 512), (D, 512), (0, 768), (D, 768), (0, 0))
VMEM_LIMIT = 67043328 - T * (B + Q // 2) * 2 - 65536
UNITS = ((0, 0, M, 0), (0, M, M, 0)) + tuple((0, 0, Z, t) for t in range(1, 5)) + (
    tuple((1, 0, Z, t) for t in range(4)) + ((1, 0, M, 4), (1, M, M, 4)))
XFIRST = (3, 7)


def _dot(a, b):
    return jnp.dot(a, b, preferred_element_type=F32)


def _kernel(x, ga, gb, wg, wu, wd, o, wo, wq, xo, qo, dl, ql, wh,
            A, N, W, act, ys, yr, yo, gv, send, recv, loc):
    h = lax.axis_index('h')
    z = lax.axis_index('f')
    iy, ix, ic = lax.div(h, 4), lax.rem(lax.div(h, 2), 2), lax.rem(h, 2)

    def dev(kx, ky, kc):
        py = 1 - iy if ky else iy
        px = 1 - ix if kx else ix
        pc = 1 - ic if kc else ic
        return {'h': py * 4 + px * 2 + pc}

    XN, YN, CN, YCN, ZN = dev(1, 0, 0), dev(0, 1, 0), dev(0, 0, 1), dev(0, 1, 1), {'f': 1 - z}
    count = [0, 0]
    sends, every = [], []

    def put(src, dst, to):
        i = count[0]
        count[0] += 1
        if i >= NSEND:
            settle([c for c in sends if c is every[i - NSEND]])
        c = pltpu.make_async_remote_copy(src, dst, send.at[i % NSEND], recv.at[i], device_id=to, device_id_type=MESH)
        c.start()
        every.append(c)
        sends.append(c)
        return c

    def load(src, dst):
        i = count[1]
        count[1] += 1
        c = pltpu.make_async_copy(src, dst, loc.at[i % NLOCAL])
        c.start()
        return c

    def settle(cs):
        for c in cs:
            c.wait_send()
            sends[:] = [d for d in sends if d is not c]

    def al(v, m):
        return pl.multiple_of(v, m)

    def ds(start, size, m):
        return pl.ds(al(start, m), size)

    def quarter(py, pc):
        return pc * (2 * R) + py * R

    mine = quarter(iy, ic)
    zr = ds(z * Z, Z, Z)
    zo = ds((1 - z) * Z, Z, Z)

    bar = pltpu.get_barrier_semaphore()
    for k in range(1, 8):
        pl.semaphore_signal(bar, inc=1, device_id=dev(k & 1, (k >> 1) & 1, k >> 2), device_id_type=MESH)
    pl.semaphore_signal(bar, inc=1, device_id=ZN, device_id_type=MESH)
    pl.semaphore_wait(bar, 8)

    def col(p):
        return pl.ds(p * B, B)

    x4 = put(x.at[ds(quarter(iy, 1 - ic), R, R), :], A.at[:, col(4)], CN)
    x2 = put(x.at[ds(quarter(1 - iy, ic) + z * Z, Z, Z), :], A.at[zr, col(2)], YN)
    x6 = put(x.at[ds(quarter(1 - iy, 1 - ic) + z * Z, Z, Z), :], A.at[zr, col(6)], YCN)
    x1 = put(x.at[ds(mine + z * Z, Z, Z), :], A.at[zr, col(1)], XN)
    x0 = load(x.at[ds(mine, R, R), :], A.at[:, col(0)])

    def wrow(j, a, n):
        return pl.ds((j % 2) * D + a, n)

    def wref(j, a, n, c=slice(None)):
        return W.at[wrow(j, a, n), c] if j < 2 else wh.at[j - 2, pl.ds(a, n), c]

    wl, wx, wyo, wyf, wc = {}, {}, {}, {}, {}
    GC, UC = pl.ds(0, PC), pl.ds(PC, PC)

    def wcol(j, other):
        return ds(((1 - ix) if other else ix) * FX + j * PC, PC, PC)

    def w_load(j):
        c0 = wcol(j, 0)
        wl[j] = [load(wg.at[:, c0], W.at[wrow(j, 0, B), GC]), load(wu.at[:, c0], W.at[wrow(j, 0, B), UC])]

    def w_x(j):
        c1 = wcol(j, 1)
        wx[j] = [put(wg.at[:, c1], wref(j, B, B, GC), XN), put(wu.at[:, c1], wref(j, B, B, UC), XN)]

    def w_yown(j):
        if j < 2:
            for c in wl[j]:
                c.wait()
            wyo[j] = [put(wref(j, 0, B), wref(j, 2 * B, B), YN)]
            wc[j] = [put(wref(j, 0, B), wref(j, 4 * B, B), CN)]
        else:
            c0 = wcol(j, 0)
            wyo[j] = [put(wg.at[:, c0], wref(j, 2 * B, B, GC), YN), put(wu.at[:, c0], wref(j, 2 * B, B, UC), YN)]
            wc[j] = [put(wg.at[:, c0], wref(j, 4 * B, B, GC), CN), put(wu.at[:, c0], wref(j, 4 * B, B, UC), CN)]

    def w_xgot(j):
        for c in wx[j]:
            c.wait_recv()
        wyf[j] = [put(wref(j, B, B), wref(j, 3 * B, B), YN)]
        wc[j].append(put(wref(j, B, B), wref(j, 5 * B, B), CN))

    def w_block(j, k, n=1):
        return load(wref(j, k * B, n * B), W.at[wrow(j, k * B, n * B), :])

    def w_ygot(j):
        for c in wyo[j]:
            c.wait_recv()
        own = len(wc[j])
        wc[j].append(put(wref(j, 2 * B, B), wref(j, 6 * B, B), CN))
        loads = []
        if j >= 2:
            w_load(j)
            for c in wc[j][:own]:
                c.wait_recv()
            loads = wl[j] + [w_block(j, 1, 2), w_block(j, 4, 2)]
        for c in wyf[j]:
            c.wait_recv()
        wc[j].append(put(wref(j, 3 * B, B), wref(j, 7 * B, B), CN))
        if j >= 2:
            loads.append(w_block(j, 3))
        for c in wc[j] if j < 2 else wc[j][own:]:
            c.wait_recv()
        if j >= 2:
            loads.append(w_block(j, 6, 2))
        for c in loads:
            c.wait()

    w_load(0)
    w_load(1)
    w_x(0)
    gs = [put(v, gv.at[i, k], dev(k & 1, (k >> 1) & 1, k >> 2)) for k in range(1, 8) for i, v in enumerate((ga, gb))]
    gv[0, 0] = ga[...]
    gv[1, 0] = gb[...]
    w_yown(0)
    w_yown(1)

    dc = [put(wd, dl.at[1, pl.ds(0, FP), :], CN), put(wo, dl.at[1, pl.ds(FP, OC), :], CN)]
    qc0 = put(wq.at[:, ds(ix * QC, QC, QC)], ql.at[4], CN)

    x4.wait_recv()
    x5 = put(A.at[zr, col(4)], A.at[zr, col(5)], XN)
    zs = []

    def zput(p):
        zs.append(put(A.at[zr, col(p)], A.at[zr, col(p)], ZN))

    x1.wait_recv()
    zput(1)
    x2.wait_recv()
    x3 = put(A.at[zr, col(2)], A.at[zr, col(3)], XN)
    zput(2)
    x6.wait_recv()
    x7 = put(A.at[zr, col(6)], A.at[zr, col(7)], XN)
    zput(6)
    for j in range(1, PIECES):
        w_x(j)
    w_xgot(0)
    w_yown(2)
    x5.wait_recv()
    zput(5)
    x3.wait_recv()
    zput(3)
    x7.wait_recv()
    zput(7)
    for c in gs:
        c.wait_recv()
    x0.wait()
    for c in zs:
        c.wait_recv()

    def norm(row, n, gi):
        gain = jnp.concatenate([gv[gi, k, i:i + 1, :] for k in range(8) for i in range(3)], 1)

        def body(i, _):
            rows = ds(row + i * 32, 32, 32)
            v = A[rows, :].astype(F32)
            ss = jnp.sum(v * v, axis=-1, keepdims=True)
            N[rows, :] = (v * lax.rsqrt(ss / D + EPS) * gain).astype(BF)
            return 0

        lax.fori_loop(0, n // 32, body, 0)

    norm(0, R, 0)

    def gate_up(j, half):
        def body(t, _):
            rows = ds(half * Z + lax.div(t, 2) * M, M, M)
            c = lax.rem(t, 2) * M
            n = N[rows, :]
            gt = _dot(n, W[wrow(j, 0, D), ds(c, M, M)])
            up = _dot(n, W[wrow(j, 0, D), ds(PC + c, M, M)])
            act[rows, ds(j * PC + c, M, M)] = (jax.nn.silu(gt) * up).astype(BF)
            return 0

        lax.fori_loop(0, (Z // M) * (PC // M), body, 0)

    dy, dyc, dloads = {}, {}, {}

    def down_y(p):
        c = pl.ds(p * S, S)
        dy[p] = [put(wd.at[:, c], dl.at[0, pl.ds(0, FP), c], YN),
                 put(wo.at[:, c], dl.at[0, pl.ds(FP, OC), c], YN)]

    def dslot(ky, p):
        return ((ky * 3 + p) % 4) * S2

    def down_load(ky, p):
        out = []
        for kc in range(2):
            c = pl.ds(p * S, S)
            if ky == 0 and kc == 0:
                top, bot = wd, wo.at[:, c]
            else:
                k = ky + 2 * kc - 1
                top, bot = dl.at[k], dl.at[k, pl.ds(FP, OC), c]
            to = pl.ds(dslot(ky, p) + kc * S, S)
            out.append(load(top.at[ds(ix * FX, FX, FX), c], W.at[pl.ds(0, FX), to]))
            out.append(load(top.at[ds((1 - ix) * FX, FX, FX), c], W.at[pl.ds(FX, FX), to]))
            out.append(load(bot, W.at[pl.ds(FP, OC), to]))
        dloads[ky, p] = out

    def w_settle(j):
        settle(wx[j] + wyo[j] + wyf[j] + wc[j])

    acts = {}

    def act_put(j, half):
        rows = zo if half else zr
        acts[j, half] = put(act.at[rows, pl.ds(j * PC, PC)], act.at[rows, pl.ds(FX + j * PC, PC)], XN)

    for j in range(PIECES):
        if j + 1 < PIECES:
            w_xgot(j + 1)
        if j == 0:
            w_yown(3)
        if j == 2:
            w_settle(0)
            for p in range(3):
                down_y(p)
        if j == 3:
            w_settle(1)
        w_ygot(j)
        gate_up(j, 1 - z)
        if j == 0:
            settle(zs + [x1, x2, x3, x4, x5, x6, x7] + gs)
        act_put(j, 1)
        if j == 3:
            act_put(2, 0)
        gate_up(j, z)
        if j != 2:
            act_put(j, 0)

    qx = put(wq.at[:, ds((1 - ix) * QC, QC, QC)], ql.at[1], XN)
    for c in dc:
        c.wait_recv()
    for p in range(3):
        down_load(0, p)
    ol = load(o.at[ds(mine, R, R), :], N.at[:, pl.ds(0, OC)])

    rs = {}

    def step(ky, p):
        return (ky * 3 + p) * S2

    def down(ky, p, half, dst, at, i0=0, n=Z // M):
        def f(i, _):
            c = pl.ds(dslot(ky, p), S2)
            rows = ds(half * Z + i * M, M, M)
            dst[ds(i * M, M, M), pl.ds(at, S2)] = (
                _dot(act[rows, :], W[pl.ds(0, FP), c]) + _dot(N[rows, pl.ds(0, OC)], W[pl.ds(FP, OC), c]))
            return 0
        lax.fori_loop(i0, i0 + n, f, 0)

    def parts(ky, p):
        return ((0, M), (M, M)) if (ky, p) == (1, 2) else ((0, Z),)

    def down_far(ky, p):
        for c in dloads[ky, p]:
            c.wait()
        s = pl.ds(step(ky, p), S2)
        for r, n in parts(ky, p):
            down(ky, p, 1 - z, ys, step(ky, p), r // M, n // M)
            rs[ky, p, r] = put(ys.at[pl.ds(r, n), s], yr.at[pl.ds(r, n), s], ZN)

    def near(ky, p):
        return ((ky * 3 + p) % 2) * S2

    def down_near(ky, p):
        down(ky, p, z, yo, near(ky, p))

    def acol(ky, p, kc, kx=0):
        return pl.ds((2 * ky + 4 * kc + kx) * B + p * S, S)

    xx, xz, xf = {}, {}, {}

    def finish_part(ky, p, r0, n):
        rs[ky, p, r0].wait_recv()

        def f(i, _):
            r = ds(r0 + i * 64, 64, 64)
            ra = ds(z * Z + r0 + i * 64, 64, 64)
            for kc in range(2):
                c = acol(ky, p, kc)
                mine_y = yo[r, pl.ds(near(ky, p) + kc * S, S)]
                A[ra, c] = (A[ra, c].astype(F32) + (mine_y + yr[r, pl.ds(step(ky, p) + kc * S, S)])).astype(BF)
            return 0

        lax.fori_loop(0, n // 64, f, 0)
        rows = ds(z * Z + r0, n, n)
        for kc in range(2):
            xx[ky, p, kc, r0] = put(A.at[rows, acol(ky, p, kc)], A.at[rows, acol(ky, p, kc, 1)], XN)

    def finish(ky, p):
        for r0, n in parts(ky, p):
            finish_part(ky, p, r0, n)

    def z_own(ky, p):
        for kc in range(2):
            c = acol(ky, p, kc)
            xz[ky, p, kc] = put(A.at[zr, c], A.at[zr, c], ZN)

    def x_got_part(ky, p, r0):
        for kc in range(2):
            xx[ky, p, kc, r0].wait_recv()

    def x_got(ky, p):
        for r0, _ in parts(ky, p):
            x_got_part(ky, p, r0)

    def z_far(ky, p):
        for kc in range(2):
            c = acol(ky, p, kc, 1)
            xf[ky, p, kc] = put(A.at[zr, c], A.at[zr, c], ZN)

    def down_ygot(p):
        for c in dy[p]:
            c.wait_recv()
        c = pl.ds(p * S, S)
        dyc[p] = put(dl.at[0, :, c], dl.at[2, :, c], CN)

    def down_ready(p):
        dyc[p].wait_recv()
        down_load(1, p)

    ol.wait()
    for j in range(PIECES):
        acts[j, 1].wait_recv()
    for p in range(3):
        down_far(0, p)
    down_ygot(0)
    down_ready(0)
    down_far(1, 0)
    for j in range(PIECES):
        acts[j, 0].wait_recv()
    down_near(0, 0)
    down_near(0, 1)
    finish(0, 0)
    down_near(0, 2)
    finish(0, 1)
    down_near(1, 0)
    finish(0, 2)
    z_own(0, 0)
    z_own(0, 1)

    qyo, qyf, qcy, qloads = {}, {}, {}, {}

    def tile(t):
        return pl.ds(t * QT, QT)

    def qw_y(gi):
        qyo[gi] = put(wq.at[:, ds(ix * QC + gi * QT, QT, QT)], ql.at[2, :, tile(gi)], YN)
        qyf[gi] = put(ql.at[1, :, tile(gi)], ql.at[3, :, tile(gi)], YN)

    def qw_ygot(gi):
        qyo[gi].wait_recv()
        a1 = put(ql.at[2, :, tile(gi)], ql.at[6, :, tile(gi)], CN)
        qyf[gi].wait_recv()
        a2 = put(ql.at[3, :, tile(gi)], ql.at[7, :, tile(gi)], CN)
        qcy[gi] = (a1, a2)

    def slot(t, k):
        r, c = QSLOT[t]
        return W.at[pl.ds(r + k * B, B), pl.ds(c, QT)]

    def qload(t, ks):
        for k in ks:
            src = ql.at[k, :, tile(t)] if k else wq.at[:, ds(ix * QC + t * QT, QT, QT)]
            qloads.setdefault(t, []).append(load(src, slot(t, k)))

    qx.wait_recv()
    qc1 = put(ql.at[1], ql.at[5], CN)
    for gi in range(QN):
        qw_y(gi)
    qc0.wait_recv()
    qc1.wait_recv()
    for gi in range(4):
        qload(gi, EARLY)

    down_ygot(1)
    down_ready(1)
    down_far(1, 1)
    z_own(0, 2)
    x_got(0, 0)
    z_far(0, 0)
    finish(1, 0)
    down_near(1, 1)
    qload(4, EARLY)
    x_got(0, 1)
    x_got(0, 2)
    finish(1, 1)
    down_ygot(2)
    down_ready(2)
    down_far(1, 2)
    z_far(0, 1)
    z_far(0, 2)
    for p in range(2):
        z_own(1, p)
    for p in range(2):
        x_got(1, p)
        z_far(1, p)
    down_near(1, 2)
    def qw_ready(gi):
        for c in qcy[gi]:
            c.wait_recv()
        qload(gi, LATE)

    qw_ygot(0)
    qw_ready(0)

    qxr, qyr, qdr, qcr = {}, {}, {}, []

    def at(u, fy, fx):
        far, r, n, t = UNITS[u]
        half = 1 - z if far else z
        py = 1 - iy if fy else iy
        px = 1 - ix if fx else ix
        return qo.at[ds(quarter(py, ic) + half * Z + r, n, n), ds(px * QC + t * QT, QT, QT)]

    def unit(u):
        far, r0, n, t = UNITS[u]
        for c in qloads.pop(t, ()):
            c.wait()
        base = (1 - z if far else z) * Z + r0

        def f(i, _):
            r, c = QSLOT[t]
            w = W[pl.ds(r, D), pl.ds(c, QT)]
            to = qo.at[ds(mine + base + i * M, M, M), ds(ix * QC + t * QT, QT, QT)]
            to[...] = _dot(N[ds(base + i * M, M, M), :], w).astype(BF)
            return 0

        lax.fori_loop(0, n // M, f, 0)
        ref = at(u, 0, 0)
        qxr[u] = put(ref, ref, XN)
        qyr[u] = put(ref, ref, YN)
        qcr.append(put(ref, ref, CN))

    def got_x(*us):
        for u in us:
            qxr[u].wait_recv()
            ref = at(u, 0, 1)
            if u in XFIRST:
                qdr[u] = put(ref, ref, YN)
            qcr.append(put(ref, ref, CN))

    def got_y(*us):
        for u in us:
            qyr[u].wait_recv()
            ref = at(u, 1, 0)
            if u not in XFIRST:
                qdr[u] = put(ref, ref, XN)
            qcr.append(put(ref, ref, CN))

    def got_d(*us):
        for u in us:
            qdr[u].wait_recv()
            ref = at(u, 1, 1)
            qcr.append(put(ref, ref, CN))

    finish(1, 2)
    z_own(1, 2)
    x_got_part(1, 2, 0)
    qw_ygot(1)
    norm(z * Z, M, 1)
    unit(0)
    qw_ready(1)
    x_got_part(1, 2, M)
    z_far(1, 2)
    norm(z * Z + M, M, 1)
    unit(1)
    unit(2)
    qw_ygot(2)
    qw_ready(2)
    got_x(0, 1)
    unit(3)
    qw_ygot(3)
    qw_ready(3)
    unit(4)
    got_x(2)
    qw_ygot(4)
    qw_ready(4)
    unit(5)
    orow = ds(mine + z * Z, Z, Z)
    oy = put(A.at[zr, col(2)], xo.at[orow, :], YN)
    oyc = put(A.at[zr, col(6)], xo.at[orow, :], YCN)
    got_x(3)
    got_y(0, 1)
    got_x(4)
    got_y(2, 3)
    got_x(5)
    got_y(4)
    for k in xz:
        xz[k].wait_recv()
    got_y(5)
    for k in xf:
        xf[k].wait_recv()
    norm((1 - z) * Z, Z, 1)
    unit(6)
    unit(7)
    unit(8)
    got_d(0, 1, 2)
    unit(9)
    unit(10)
    unit(11)
    oc = put(A.at[:, col(4)], xo.at[ds(mine, R, R), :], CN)

    def keep(i, _):
        xo[ds(mine + i * M, M, M), :] = A[ds(i * M, M, M), col(0)]
        return 0

    lax.fori_loop(0, R // M, keep, 0)
    got_x(6)
    oy.wait_recv()
    r0 = ds(quarter(1 - iy, ic) + z * Z, Z, Z)
    ozy = put(xo.at[r0, :], xo.at[r0, :], ZN)
    oyc.wait_recv()
    r1 = ds(quarter(1 - iy, 1 - ic) + z * Z, Z, Z)
    ozc = put(xo.at[r1, :], xo.at[r1, :], ZN)
    got_d(3, 4, 5)
    got_x(7)
    got_y(6)
    got_x(8)
    got_y(7)
    got_x(9)
    got_y(8)
    got_x(10, 11)
    got_y(9, 10, 11)
    got_d(*range(6, 12))
    for c in (oc, ozy, ozc):
        c.wait_recv()
    for c in qcr:
        c.wait_recv()
    settle(list(sends))


def _write(a, b, ao, bo, sem):
    jobs = [(a, ao, pl.ds(0, T))] + [(b, bo, pl.ds(i * (T // NWRITE), T // NWRITE)) for i in range(NWRITE)]
    copies = [pltpu.make_async_copy(s.at[r, :], d.at[r, :], sem.at[i]) for i, (s, d, r) in enumerate(jobs)]
    for c in copies:
        c.start()
    for c in copies:
        c.wait()


def solution(mesh):
    def body(x, g1, g2, w_gate, w_up, w_down, o, w_o, w_qkv):
        hbm, vmem = pl.BlockSpec(memory_space=pltpu.HBM), pl.BlockSpec(memory_space=pltpu.VMEM)
        keep = lambda v: pltpu.with_memory_space_constraint(v, pltpu.HBM)
        outs = pl.pallas_call(
            _kernel,
            out_shape=(pltpu.VMEM((T, B), BF), pltpu.VMEM((T, Q // 2), BF), pltpu.HBM((3, K2, B), BF),
                       pltpu.HBM((8, B, QC), BF), pltpu.HBM((2, D, 2 * PC), BF)),
            in_specs=[hbm, vmem, vmem] + [hbm] * 6,
            out_specs=(vmem, vmem, hbm, hbm, hbm),
            scratch_shapes=[
                pltpu.VMEM((R, D), BF), pltpu.VMEM((R, D), BF), pltpu.VMEM((2 * D, 2 * PC), BF),
                pltpu.VMEM((R, FP), BF), pltpu.VMEM((Z, 6 * S2), F32), pltpu.VMEM((Z, 6 * S2), F32),
                pltpu.VMEM((Z, 4 * S), F32), pltpu.VMEM((2, 8, 3, 128), F32),
                pltpu.SemaphoreType.DMA((NSEND,)), pltpu.SemaphoreType.DMA((NREMOTE,)),
                pltpu.SemaphoreType.DMA((NLOCAL,)),
            ],
            compiler_params=pltpu.CompilerParams(collective_id=0, has_side_effects=True,
                                                 vmem_limit_bytes=VMEM_LIMIT),
        )(keep(x), g1.reshape(3, 128), g2.reshape(3, 128), *[keep(v) for v in (w_gate, w_up, w_down, o, w_o, w_qkv)])
        return pl.pallas_call(
            _write,
            out_shape=tuple(jax.ShapeDtypeStruct(v.shape, v.dtype) for v in outs[:2]),
            in_specs=[vmem, vmem],
            out_specs=(hbm, hbm),
            scratch_shapes=[pltpu.SemaphoreType.DMA((NWRITE + 1,))],
            compiler_params=pltpu.CompilerParams(vmem_limit_bytes=4 * T * D // 12),
        )(*[pltpu.with_memory_space_constraint(v, pltpu.VMEM) for v in outs[:2]])

    in_specs = (P(None, 'h'), P('h'), P('h'), P('h', 'f'), P('h', 'f'), P('f', 'h'),
                P(None, 'f'), P('f', 'h'), P('h', 'f'))
    return jax.shard_map(body, mesh=mesh, in_specs=in_specs,
                         out_specs=(P(None, 'h'), P(None, 'f')), check_vma=False)
```

```python
import jax
import jax.numpy as jnp
from jax import lax
from jax.experimental import pallas as pl
from jax.experimental.pallas import tpu as pltpu
from jax.sharding import PartitionSpec as P

EPS = 1e-6
BF, F32 = jnp.bfloat16, jnp.float32
MESH = pl.DeviceIdType.MESH
NREMOTE, NSEND, NLOCAL, NWRITE = 239, 64, 48, 8

T, D, FF, HD, Q = 4096, 3072, 8192, 3072, 5120
B = D // 8
R = T // 4
Z = R // 2
FP = FF // 2
PIECES = 4
PC = FP // 2 // PIECES
K2 = FP + HD // 2
S = 128
QC = Q // 4
M = 256
FX, OC, S2 = FP // 2, HD // 2, 2 * S
QT = 256
QN = QC // QT
EARLY, LATE = (0, 1, 4, 5), (2, 3, 6, 7)
QSLOT = ((0, 512), (D, 512), (0, 768), (D, 768), (0, 0))
VMEM_LIMIT = 67043328 - T * (B + Q // 2) * 2 - 65536
UNITS = ((0, 0, M, 0), (0, M, M, 0)) + tuple((0, 0, Z, t) for t in range(1, 5)) + (
    tuple((1, 0, Z, t) for t in range(4)) + ((1, 0, M, 4), (1, M, M, 4)))
XFIRST = (3, 7)


def _dot(a, b):
    return jnp.dot(a, b, preferred_element_type=F32)


def _kernel(x, ga, gb, wg, wu, wd, o, wo, wq, xo, qo, dl, ql, wh,
            A, N, W, act, ys, yr, yo, gv, send, recv, loc):
    h = lax.axis_index('h')
    z = lax.axis_index('f')
    iy, ix, ic = lax.div(h, 4), lax.rem(lax.div(h, 2), 2), lax.rem(h, 2)

    def dev(kx, ky, kc):
        py = 1 - iy if ky else iy
        px = 1 - ix if kx else ix
        pc = 1 - ic if kc else ic
        return {'h': py * 4 + px * 2 + pc}

    XN, YN, CN, YCN, ZN = dev(1, 0, 0), dev(0, 1, 0), dev(0, 0, 1), dev(0, 1, 1), {'f': 1 - z}
    count = [0, 0]
    sends, every = [], []

    def put(src, dst, to):
        i = count[0]
        count[0] += 1
        if i >= NSEND:
            settle([c for c in sends if c is every[i - NSEND]])
        c = pltpu.make_async_remote_copy(src, dst, send.at[i % NSEND], recv.at[i], device_id=to, device_id_type=MESH)
        c.start()
        every.append(c)
        sends.append(c)
        return c

    def load(src, dst):
        i = count[1]
        count[1] += 1
        c = pltpu.make_async_copy(src, dst, loc.at[i % NLOCAL])
        c.start()
        return c

    def settle(cs):
        for c in cs:
            c.wait_send()
            sends[:] = [d for d in sends if d is not c]

    def al(v, m):
        return pl.multiple_of(v, m)

    def ds(start, size, m):
        return pl.ds(al(start, m), size)

    def quarter(py, pc):
        return pc * (2 * R) + py * R

    mine = quarter(iy, ic)
    zr = ds(z * Z, Z, Z)
    zo = ds((1 - z) * Z, Z, Z)

    bar = pltpu.get_barrier_semaphore()
    for k in range(1, 8):
        pl.semaphore_signal(bar, inc=1, device_id=dev(k & 1, (k >> 1) & 1, k >> 2), device_id_type=MESH)
    pl.semaphore_signal(bar, inc=1, device_id=ZN, device_id_type=MESH)
    pl.semaphore_wait(bar, 8)

    def col(p):
        return pl.ds(p * B, B)

    x4 = put(x.at[ds(quarter(iy, 1 - ic), R, R), :], A.at[:, col(4)], CN)
    x2 = put(x.at[ds(quarter(1 - iy, ic) + z * Z, Z, Z), :], A.at[zr, col(2)], YN)
    x6 = put(x.at[ds(quarter(1 - iy, 1 - ic) + z * Z, Z, Z), :], A.at[zr, col(6)], YCN)
    x1 = put(x.at[ds(mine + z * Z, Z, Z), :], A.at[zr, col(1)], XN)
    x0 = load(x.at[ds(mine, R, R), :], A.at[:, col(0)])

    def wrow(j, a, n):
        return pl.ds((j % 2) * D + a, n)

    def wref(j, a, n, c=slice(None)):
        return W.at[wrow(j, a, n), c] if j < 2 else wh.at[j - 2, pl.ds(a, n), c]

    wl, wx, wyo, wyf, wc = {}, {}, {}, {}, {}
    GC, UC = pl.ds(0, PC), pl.ds(PC, PC)

    def wcol(j, other):
        return ds(((1 - ix) if other else ix) * FX + j * PC, PC, PC)

    def w_load(j):
        c0 = wcol(j, 0)
        wl[j] = [load(wg.at[:, c0], W.at[wrow(j, 0, B), GC]), load(wu.at[:, c0], W.at[wrow(j, 0, B), UC])]

    def w_x(j):
        c1 = wcol(j, 1)
        wx[j] = [put(wg.at[:, c1], wref(j, B, B, GC), XN), put(wu.at[:, c1], wref(j, B, B, UC), XN)]

    def w_yown(j):
        if j < 2:
            for c in wl[j]:
                c.wait()
            wyo[j] = [put(wref(j, 0, B), wref(j, 2 * B, B), YN)]
            wc[j] = [put(wref(j, 0, B), wref(j, 4 * B, B), CN)]
        else:
            c0 = wcol(j, 0)
            wyo[j] = [put(wg.at[:, c0], wref(j, 2 * B, B, GC), YN), put(wu.at[:, c0], wref(j, 2 * B, B, UC), YN)]
            wc[j] = [put(wg.at[:, c0], wref(j, 4 * B, B, GC), CN), put(wu.at[:, c0], wref(j, 4 * B, B, UC), CN)]

    def w_xgot(j):
        for c in wx[j]:
            c.wait_recv()
        wyf[j] = [put(wref(j, B, B), wref(j, 3 * B, B), YN)]
        wc[j].append(put(wref(j, B, B), wref(j, 5 * B, B), CN))

    def w_block(j, k, n=1):
        return load(wref(j, k * B, n * B), W.at[wrow(j, k * B, n * B), :])

    def w_ygot(j):
        for c in wyo[j]:
            c.wait_recv()
        own = len(wc[j])
        wc[j].append(put(wref(j, 2 * B, B), wref(j, 6 * B, B), CN))
        loads = []
        if j >= 2:
            w_load(j)
            for c in wc[j][:own]:
                c.wait_recv()
            loads = wl[j] + [w_block(j, 1, 2), w_block(j, 4, 2)]
        for c in wyf[j]:
            c.wait_recv()
        wc[j].append(put(wref(j, 3 * B, B), wref(j, 7 * B, B), CN))
        if j >= 2:
            loads.append(w_block(j, 3))
        for c in wc[j] if j < 2 else wc[j][own:]:
            c.wait_recv()
        if j >= 2:
            loads.append(w_block(j, 6, 2))
        for c in loads:
            c.wait()

    w_load(0)
    w_load(1)
    w_x(0)
    gs = [put(v, gv.at[i, k], dev(k & 1, (k >> 1) & 1, k >> 2)) for k in range(1, 8) for i, v in enumerate((ga, gb))]
    gv[0, 0] = ga[...]
    gv[1, 0] = gb[...]
    w_yown(0)
    w_yown(1)

    dc = [put(wd, dl.at[1, pl.ds(0, FP), :], CN), put(wo, dl.at[1, pl.ds(FP, OC), :], CN)]
    qc0 = put(wq.at[:, ds(ix * QC, QC, QC)], ql.at[4], CN)

    x4.wait_recv()
    x5 = put(A.at[zr, col(4)], A.at[zr, col(5)], XN)
    zs = []

    def zput(p):
        zs.append(put(A.at[zr, col(p)], A.at[zr, col(p)], ZN))

    x1.wait_recv()
    zput(1)
    x2.wait_recv()
    x3 = put(A.at[zr, col(2)], A.at[zr, col(3)], XN)
    zput(2)
    x6.wait_recv()
    x7 = put(A.at[zr, col(6)], A.at[zr, col(7)], XN)
    zput(6)
    for j in range(1, PIECES):
        w_x(j)
    w_xgot(0)
    w_yown(2)
    x5.wait_recv()
    zput(5)
    x3.wait_recv()
    zput(3)
    x7.wait_recv()
    zput(7)
    for c in gs:
        c.wait_recv()
    x0.wait()
    for c in zs:
        c.wait_recv()

    def norm(row, n, gi):
        gain = jnp.concatenate([gv[gi, k, i:i + 1, :] for k in range(8) for i in range(3)], 1)

        def body(i, _):
            rows = ds(row + i * 32, 32, 32)
            v = A[rows, :].astype(F32)
            ss = jnp.sum(v * v, axis=-1, keepdims=True)
            N[rows, :] = (v * lax.rsqrt(ss / D + EPS) * gain).astype(BF)
            return 0

        lax.fori_loop(0, n // 32, body, 0)

    norm(0, R, 0)

    def gate_up(j, half):
        def body(t, _):
            rows = ds(half * Z + lax.div(t, 2) * M, M, M)
            c = lax.rem(t, 2) * M
            n = N[rows, :]
            gt = _dot(n, W[wrow(j, 0, D), ds(c, M, M)])
            up = _dot(n, W[wrow(j, 0, D), ds(PC + c, M, M)])
            act[rows, ds(j * PC + c, M, M)] = (jax.nn.silu(gt) * up).astype(BF)
            return 0

        lax.fori_loop(0, (Z // M) * (PC // M), body, 0)

    dy, dyc, dloads = {}, {}, {}

    def down_y(p):
        c = pl.ds(p * S, S)
        dy[p] = [put(wd.at[:, c], dl.at[0, pl.ds(0, FP), c], YN),
                 put(wo.at[:, c], dl.at[0, pl.ds(FP, OC), c], YN)]

    def dslot(ky, p):
        return ((ky * 3 + p) % 4) * S2

    def down_load(ky, p):
        out = []
        for kc in range(2):
            c = pl.ds(p * S, S)
            if ky == 0 and kc == 0:
                top, bot = wd, wo.at[:, c]
            else:
                k = ky + 2 * kc - 1
                top, bot = dl.at[k], dl.at[k, pl.ds(FP, OC), c]
            to = pl.ds(dslot(ky, p) + kc * S, S)
            out.append(load(top.at[ds(ix * FX, FX, FX), c], W.at[pl.ds(0, FX), to]))
            out.append(load(top.at[ds((1 - ix) * FX, FX, FX), c], W.at[pl.ds(FX, FX), to]))
            out.append(load(bot, W.at[pl.ds(FP, OC), to]))
        dloads[ky, p] = out

    def w_settle(j):
        settle(wx[j] + wyo[j] + wyf[j] + wc[j])

    acts = {}

    def act_put(j, half):
        rows = zo if half else zr
        acts[j, half] = put(act.at[rows, pl.ds(j * PC, PC)], act.at[rows, pl.ds(FX + j * PC, PC)], XN)

    for j in range(PIECES):
        if j + 1 < PIECES:
            w_xgot(j + 1)
        if j == 0:
            w_yown(3)
        if j == 2:
            w_settle(0)
            for p in range(3):
                down_y(p)
        if j == 3:
            w_settle(1)
        w_ygot(j)
        gate_up(j, 1 - z)
        if j == 0:
            settle(zs + [x1, x2, x3, x4, x5, x6, x7] + gs)
        act_put(j, 1)
        if j == 3:
            act_put(2, 0)
        gate_up(j, z)
        if j != 2:
            act_put(j, 0)

    qx = put(wq.at[:, ds((1 - ix) * QC, QC, QC)], ql.at[1], XN)
    for c in dc:
        c.wait_recv()
    for p in range(3):
        down_load(0, p)
    ol = load(o.at[ds(mine, R, R), :], N.at[:, pl.ds(0, OC)])

    rs = {}

    def step(ky, p):
        return (ky * 3 + p) * S2

    def down(ky, p, half, dst, at, i0=0, n=Z // M):
        def f(i, _):
            c = pl.ds(dslot(ky, p), S2)
            rows = ds(half * Z + i * M, M, M)
            dst[ds(i * M, M, M), pl.ds(at, S2)] = (
                _dot(act[rows, :], W[pl.ds(0, FP), c]) + _dot(N[rows, pl.ds(0, OC)], W[pl.ds(FP, OC), c]))
            return 0
        lax.fori_loop(i0, i0 + n, f, 0)

    def parts(ky, p):
        return ((0, M), (M, M)) if (ky, p) == (1, 2) else ((0, Z),)

    def down_far(ky, p):
        for c in dloads[ky, p]:
            c.wait()
        s = pl.ds(step(ky, p), S2)
        for r, n in parts(ky, p):
            down(ky, p, 1 - z, ys, step(ky, p), r // M, n // M)
            rs[ky, p, r] = put(ys.at[pl.ds(r, n), s], yr.at[pl.ds(r, n), s], ZN)

    def near(ky, p):
        return ((ky * 3 + p) % 2) * S2

    def down_near(ky, p):
        down(ky, p, z, yo, near(ky, p))

    def acol(ky, p, kc, kx=0):
        return pl.ds((2 * ky + 4 * kc + kx) * B + p * S, S)

    xx, xz, xf = {}, {}, {}

    def finish_part(ky, p, r0, n):
        rs[ky, p, r0].wait_recv()

        def f(i, _):
            r = ds(r0 + i * 64, 64, 64)
            ra = ds(z * Z + r0 + i * 64, 64, 64)
            for kc in range(2):
                c = acol(ky, p, kc)
                mine_y = yo[r, pl.ds(near(ky, p) + kc * S, S)]
                A[ra, c] = (A[ra, c].astype(F32) + (mine_y + yr[r, pl.ds(step(ky, p) + kc * S, S)])).astype(BF)
            return 0

        lax.fori_loop(0, n // 64, f, 0)
        rows = ds(z * Z + r0, n, n)
        for kc in range(2):
            xx[ky, p, kc, r0] = put(A.at[rows, acol(ky, p, kc)], A.at[rows, acol(ky, p, kc, 1)], XN)

    def finish(ky, p):
        for r0, n in parts(ky, p):
            finish_part(ky, p, r0, n)

    def z_own(ky, p):
        for kc in range(2):
            c = acol(ky, p, kc)
            xz[ky, p, kc] = put(A.at[zr, c], A.at[zr, c], ZN)

    def x_got_part(ky, p, r0):
        for kc in range(2):
            xx[ky, p, kc, r0].wait_recv()

    def x_got(ky, p):
        for r0, _ in parts(ky, p):
            x_got_part(ky, p, r0)

    def z_far(ky, p):
        for kc in range(2):
            c = acol(ky, p, kc, 1)
            xf[ky, p, kc] = put(A.at[zr, c], A.at[zr, c], ZN)

    def down_ygot(p):
        for c in dy[p]:
            c.wait_recv()
        c = pl.ds(p * S, S)
        dyc[p] = put(dl.at[0, :, c], dl.at[2, :, c], CN)

    def down_ready(p):
        dyc[p].wait_recv()
        down_load(1, p)

    ol.wait()
    for j in range(PIECES):
        acts[j, 1].wait_recv()
    for p in range(3):
        down_far(0, p)
    down_ygot(0)
    down_ready(0)
    down_far(1, 0)
    for j in range(PIECES):
        acts[j, 0].wait_recv()
    down_near(0, 0)
    down_near(0, 1)
    finish(0, 0)
    down_near(0, 2)
    finish(0, 1)
    down_near(1, 0)
    finish(0, 2)
    z_own(0, 0)
    z_own(0, 1)

    qyo, qyf, qcy, qloads = {}, {}, {}, {}

    def tile(t):
        return pl.ds(t * QT, QT)

    def qw_y(gi):
        qyo[gi] = put(wq.at[:, ds(ix * QC + gi * QT, QT, QT)], ql.at[2, :, tile(gi)], YN)
        qyf[gi] = put(ql.at[1, :, tile(gi)], ql.at[3, :, tile(gi)], YN)

    def qw_ygot(gi):
        qyo[gi].wait_recv()
        a1 = put(ql.at[2, :, tile(gi)], ql.at[6, :, tile(gi)], CN)
        qyf[gi].wait_recv()
        a2 = put(ql.at[3, :, tile(gi)], ql.at[7, :, tile(gi)], CN)
        qcy[gi] = (a1, a2)

    def slot(t, k):
        r, c = QSLOT[t]
        return W.at[pl.ds(r + k * B, B), pl.ds(c, QT)]

    def qload(t, ks):
        for k in ks:
            src = ql.at[k, :, tile(t)] if k else wq.at[:, ds(ix * QC + t * QT, QT, QT)]
            qloads.setdefault(t, []).append(load(src, slot(t, k)))

    qx.wait_recv()
    qc1 = put(ql.at[1], ql.at[5], CN)
    for gi in range(QN):
        qw_y(gi)
    qc0.wait_recv()
    qc1.wait_recv()
    for gi in range(4):
        qload(gi, EARLY)

    down_ygot(1)
    down_ready(1)
    down_far(1, 1)
    z_own(0, 2)
    x_got(0, 0)
    z_far(0, 0)
    finish(1, 0)
    down_near(1, 1)
    qload(4, EARLY)
    x_got(0, 1)
    x_got(0, 2)
    finish(1, 1)
    down_ygot(2)
    down_ready(2)
    down_far(1, 2)
    z_far(0, 1)
    z_far(0, 2)
    for p in range(2):
        z_own(1, p)
    for p in range(2):
        x_got(1, p)
        z_far(1, p)
    down_near(1, 2)
    def qw_ready(gi):
        for c in qcy[gi]:
            c.wait_recv()
        qload(gi, LATE)

    qw_ygot(0)
    qw_ready(0)

    qxr, qyr, qdr, qcr = {}, {}, {}, []

    def at(u, fy, fx):
        far, r, n, t = UNITS[u]
        half = 1 - z if far else z
        py = 1 - iy if fy else iy
        px = 1 - ix if fx else ix
        return qo.at[ds(quarter(py, ic) + half * Z + r, n, n), ds(px * QC + t * QT, QT, QT)]

    def unit(u):
        far, r0, n, t = UNITS[u]
        for c in qloads.pop(t, ()):
            c.wait()
        base = (1 - z if far else z) * Z + r0

        def f(i, _):
            r, c = QSLOT[t]
            w = W[pl.ds(r, D), pl.ds(c, QT)]
            to = qo.at[ds(mine + base + i * M, M, M), ds(ix * QC + t * QT, QT, QT)]
            to[...] = _dot(N[ds(base + i * M, M, M), :], w).astype(BF)
            return 0

        lax.fori_loop(0, n // M, f, 0)
        ref = at(u, 0, 0)
        qxr[u] = put(ref, ref, XN)
        qyr[u] = put(ref, ref, YN)
        qcr.append(put(ref, ref, CN))

    def got_x(*us):
        for u in us:
            qxr[u].wait_recv()
            ref = at(u, 0, 1)
            if u in XFIRST:
                qdr[u] = put(ref, ref, YN)
            qcr.append(put(ref, ref, CN))

    def got_y(*us):
        for u in us:
            qyr[u].wait_recv()
            ref = at(u, 1, 0)
            if u not in XFIRST:
                qdr[u] = put(ref, ref, XN)
            qcr.append(put(ref, ref, CN))

    def got_d(*us):
        for u in us:
            qdr[u].wait_recv()
            ref = at(u, 1, 1)
            qcr.append(put(ref, ref, CN))

    finish(1, 2)
    z_own(1, 2)
    x_got_part(1, 2, 0)
    qw_ygot(1)
    norm(z * Z, M, 1)
    unit(0)
    qw_ready(1)
    x_got_part(1, 2, M)
    z_far(1, 2)
    norm(z * Z + M, M, 1)
    unit(1)
    unit(2)
    qw_ygot(2)
    qw_ready(2)
    got_x(0, 1)
    unit(3)
    qw_ygot(3)
    qw_ready(3)
    unit(4)
    got_x(2)
    qw_ygot(4)
    qw_ready(4)
    unit(5)
    orow = ds(mine + z * Z, Z, Z)
    oy = put(A.at[zr, col(2)], xo.at[orow, :], YN)
    oyc = put(A.at[zr, col(6)], xo.at[orow, :], YCN)
    got_x(3)
    got_y(0, 1)
    got_x(4)
    got_y(2, 3)
    got_x(5)
    got_y(4)
    for k in xz:
        xz[k].wait_recv()
    got_y(5)
    for k in xf:
        xf[k].wait_recv()
    norm((1 - z) * Z, Z, 1)
    unit(6)
    unit(7)
    unit(8)
    got_d(0, 1, 2)
    unit(9)
    unit(10)
    unit(11)
    oc = put(A.at[:, col(4)], xo.at[ds(mine, R, R), :], CN)

    def keep(i, _):
        xo[ds(mine + i * M, M, M), :] = A[ds(i * M, M, M), col(0)]
        return 0

    lax.fori_loop(0, R // M, keep, 0)
    got_x(6)
    oy.wait_recv()
    r0 = ds(quarter(1 - iy, ic) + z * Z, Z, Z)
    ozy = put(xo.at[r0, :], xo.at[r0, :], ZN)
    oyc.wait_recv()
    r1 = ds(quarter(1 - iy, 1 - ic) + z * Z, Z, Z)
    ozc = put(xo.at[r1, :], xo.at[r1, :], ZN)
    got_d(3, 4, 5)
    got_x(7)
    got_y(6)
    got_x(8)
    got_y(7)
    got_x(9)
    got_y(8)
    got_x(10, 11)
    got_y(9, 10, 11)
    got_d(*range(6, 12))
    for c in (oc, ozy, ozc):
        c.wait_recv()
    for c in qcr:
        c.wait_recv()
    settle(list(sends))


def _write(a, b, ao, bo, sem):
    jobs = [(a, ao, pl.ds(0, T))] + [(b, bo, pl.ds(i * (T // NWRITE), T // NWRITE)) for i in range(NWRITE)]
    copies = [pltpu.make_async_copy(s.at[r, :], d.at[r, :], sem.at[i]) for i, (s, d, r) in enumerate(jobs)]
    for c in copies:
        c.start()
    for c in copies:
        c.wait()


def solution(mesh):
    def body(x, g1, g2, w_gate, w_up, w_down, o, w_o, w_qkv):
        hbm, vmem = pl.BlockSpec(memory_space=pltpu.HBM), pl.BlockSpec(memory_space=pltpu.VMEM)
        keep = lambda v: pltpu.with_memory_space_constraint(v, pltpu.HBM)
        outs = pl.pallas_call(
            _kernel,
            out_shape=(pltpu.VMEM((T, B), BF), pltpu.VMEM((T, Q // 2), BF), pltpu.HBM((3, K2, B), BF),
                       pltpu.HBM((8, B, QC), BF), pltpu.HBM((2, D, 2 * PC), BF)),
            in_specs=[hbm, vmem, vmem] + [hbm] * 6,
            out_specs=(vmem, vmem, hbm, hbm, hbm),
            scratch_shapes=[
                pltpu.VMEM((R, D), BF), pltpu.VMEM((R, D), BF), pltpu.VMEM((2 * D, 2 * PC), BF),
                pltpu.VMEM((R, FP), BF), pltpu.VMEM((Z, 6 * S2), F32), pltpu.VMEM((Z, 6 * S2), F32),
                pltpu.VMEM((Z, 4 * S), F32), pltpu.VMEM((2, 8, 3, 128), F32),
                pltpu.SemaphoreType.DMA((NSEND,)), pltpu.SemaphoreType.DMA((NREMOTE,)),
                pltpu.SemaphoreType.DMA((NLOCAL,)),
            ],
            compiler_params=pltpu.CompilerParams(collective_id=0, has_side_effects=True,
                                                 vmem_limit_bytes=VMEM_LIMIT),
        )(keep(x), g1.reshape(3, 128), g2.reshape(3, 128), *[keep(v) for v in (w_gate, w_up, w_down, o, w_o, w_qkv)])
        return pl.pallas_call(
            _write,
            out_shape=tuple(jax.ShapeDtypeStruct(v.shape, v.dtype) for v in outs[:2]),
            in_specs=[vmem, vmem],
            out_specs=(hbm, hbm),
            scratch_shapes=[pltpu.SemaphoreType.DMA((NWRITE + 1,))],
            compiler_params=pltpu.CompilerParams(vmem_limit_bytes=4 * T * D // 12),
        )(*[pltpu.with_memory_space_constraint(v, pltpu.VMEM) for v in outs[:2]])

    in_specs = (P(None, 'h'), P('h'), P('h'), P('h', 'f'), P('h', 'f'), P('f', 'h'),
                P(None, 'f'), P('f', 'h'), P('h', 'f'))
    return jax.shard_map(body, mesh=mesh, in_specs=in_specs,
                         out_specs=(P(None, 'h'), P(None, 'f')), check_vma=False)
```
